32 devices in a mesh: clients: 8 (over z, x), shard: 4 (over y, core).
Axes of the slice: x: 2, y: 2, z: 4, core: 2. Of those that a mesh axis runs over, the one named last changes fastest.
Arguments:
- quantized: int32 [8, 2097152], P('clients', 'shard'), may hold values from 0 to 2097151
- pair_masks: int32 [8, 2097152], P('clients', 'shard'), may hold values from 0 to 2097142, as said below
- alive_flags: int32 [8], P('clients'), may hold values from 0 to 1, as said below
- row_seeds: int32 [64], replicated, may hold values from 0 to 1073741823
Outputs:
- aggregate: int32 [2097152], P('shard')
- commitments: int32 [8, 64], P('clients')
- mismatch: int32 [64], replicated
The draws below stay inside these ranges and needn't reach their ends.
Inputs may be any that keep to these rules, and one draw needn't show every extreme that they name: For every position, the pair_masks of all 8 participants sum to a multiple of 2097143. `alive_flags`: at least one participant has flag 1 and at least one has flag 0.
All inputs are finite; a program needn't handle non-finite values.
Results may differ from the reference program's by a relative error of at most 0.000001.
Values may be sent and summed in bfloat16 or wider, within the bound.
A program may use at most 64 MiB of HBM per device.

```python
import math
import jax
import jax.numpy as jnp
from jax import lax

ROWS = 64
CLIENTS = 8
L = 2097152


def draw_pair_masks(key, part):
    drawn_base = jax.random.randint(jax.random.fold_in(key, 11), (CLIENTS, L), 0, 2097143, dtype=jnp.int32)
    following = jnp.roll(drawn_base, -1, axis=0)
    return (drawn_base - following) % 2097143


def draw_alive_flags(key, part):
    drawn_bits = jax.random.randint(jax.random.fold_in(key, 23), (CLIENTS,), 0, 2, dtype=jnp.int32)
    chosen = jax.random.randint(jax.random.fold_in(key, 29), (), 0, CLIENTS, dtype=jnp.int32)
    position = jnp.arange(CLIENTS, dtype=jnp.int32)
    drawn_bits = jnp.where(position == chosen, 0, drawn_bits)
    return jnp.where(position == (chosen + 1) % CLIENTS, 1, drawn_bits).astype(jnp.int32)


def with_ends(values, rng, least, largest):
    longest = values.shape.index(max(values.shape))
    spots = []
    for shift in (0, 1):
        where = [jax.random.randint(jax.random.fold_in(rng, axis), (), 0, length) for axis, length in enumerate(values.shape)]
        where[longest] = (where[longest] + shift) % values.shape[longest]
        spots.append(tuple(where))
    return values.at[spots[0]].set(least).at[spots[1]].set(largest)


def setup_inputs(seed: int = 0) -> dict:
    seeds = jax.random.split(jax.random.key(seed), 5)
    quantized = with_ends(jax.random.randint(seeds[0], (CLIENTS, L), 0, 2097152), jax.random.fold_in(seeds[0], 1), 0, 2097151).astype(jnp.int32)
    pair_masks = draw_pair_masks(jax.random.fold_in(seeds[4], 71), 0)
    alive_flags = draw_alive_flags(jax.random.fold_in(seeds[4], 71), 0)
    row_seeds = with_ends(jax.random.randint(seeds[3], (ROWS,), 0, 1073741824), jax.random.fold_in(seeds[3], 1), 0, 1073741823).astype(jnp.int32)
    return dict(quantized=quantized, pair_masks=pair_masks, alive_flags=alive_flags, row_seeds=row_seeds)


modulus = 2097143


def table_entries(row_seeds, columns):
    mixed = columns[None, :] * 747796405 + row_seeds[:, None]
    mixed = mixed & 2147483647
    mixed = mixed ^ (mixed >> 15)
    mixed = (mixed * 277803737) & 2147483647
    mixed = mixed ^ (mixed >> 13)
    mixed = (mixed * 1103515245) & 2147483647
    mixed = mixed ^ (mixed >> 16)
    return mixed & 1023


def project_mod(row_seeds, vectors, offset, block_width):
    vec_count = vectors.shape[0]
    length = vectors.shape[1]
    row_count = row_seeds.shape[0]
    sub_width = math.gcd(block_width, 512)
    block_count = length // block_width

    def advance(running, block_index):
        start_col = block_index * block_width
        columns = offset + start_col + jnp.arange(block_width, dtype=jnp.int32)
        table = table_entries(row_seeds, columns)
        right_part = lax.dynamic_slice_in_dim(vectors, start_col, block_width, 1)
        products = (right_part[:, None, :] * table[None, :, :]) % modulus
        products = products.reshape(vec_count, row_count, block_width // sub_width, sub_width)
        partial_value = jnp.sum(products, axis=3, dtype=jnp.int32) % modulus
        partial_value = jnp.sum(partial_value, axis=2, dtype=jnp.int32) % modulus
        return (running + partial_value) % modulus, None

    running = jnp.zeros((vec_count, row_count), jnp.int32)
    running, unused = lax.scan(advance, running, jnp.arange(block_count, dtype=jnp.int32))
    return running


def reference(quantized, pair_masks, alive_flags, row_seeds):
    masked = ((quantized + pair_masks) % modulus) * alive_flags[:, None]
    aggregate = jnp.sum(masked, axis=0, dtype=jnp.int32) % modulus
    col_block = math.gcd(quantized.shape[1], 4096)
    commitments = project_mod(row_seeds, quantized, 0, col_block)
    expected = jnp.sum(commitments * alive_flags[:, None], axis=0, dtype=jnp.int32) % modulus
    projected = project_mod(row_seeds, aggregate[None, :], 0, col_block)[0]
    mismatch = (projected - expected) % modulus
    return aggregate, commitments, mismatch
```

```python
import functools

import jax
import jax.numpy as jnp
from jax import lax
from jax.experimental import pallas as pl
from jax.experimental.pallas import tpu as pltpu
from jax.sharding import PartitionSpec as P

modulus = 2097143
mask21 = 2097151
LANES = 128
STREAMS = 4
AHEAD = 3
STRIDE = (LANES * 747796405 + 2147483648) % 4294967296 - 2147483648


def reduce_mod(x):
    x = (x & mask21) + (x >> 21) * 9
    return jnp.where(x >= modulus, x - modulus, x)


def wrap_once(x):
    return jnp.where(x >= modulus, x - modulus, x)


def packed_rows(count):
    tiles = count // 8
    return 8 * (2 * (tiles // 3) + tiles % 3)


def pack3(a, b, c):
    return a | (c << 21), b | ((c >> 11) << 21)


def unpack3(x, y):
    c = lax.shift_right_logical(x, 21) | ((y >> 21) << 11)
    return x & mask21, y & mask21, c


def each_step(tiles, fn):
    step = max(d for d in range(1, 9) if tiles % d == 0)

    def one(i):
        fn(i * step * 8, step * 8)

    if tiles == step:
        one(0)
    else:
        pl.loop(0, tiles // step)(one)


def pack_block(src, start, dst, at, count):
    third = 8 * (count // 24)
    rest = count - 3 * third

    def rows(x):
        return pl.multiple_of(x, 8)

    if third:

        def one(i, n):
            a = src[pl.ds(rows(start + i), n), :]
            b = src[pl.ds(rows(start + third + i), n), :]
            c = src[pl.ds(rows(start + 2 * third + i), n), :]
            x, y = pack3(a, b, c)
            dst[pl.ds(rows(at + i), n), :] = x
            dst[pl.ds(rows(at + third + i), n), :] = y

        each_step(third // 8, one)
    if rest:
        dst[pl.ds(rows(at + 2 * third), rest), :] = src[pl.ds(rows(start + 3 * third), rest), :]


def unpack_block(src, at, count, put):
    third = 8 * (count // 24)
    rest = count - 3 * third

    def rows(x):
        return pl.multiple_of(x, 8)

    if third:

        def one(i, n):
            x = src[pl.ds(rows(at + i), n), :]
            y = src[pl.ds(rows(at + third + i), n), :]
            for j, v in enumerate(unpack3(x, y)):
                put(j * third + i, n, v)

        each_step(third // 8, one)
    if rest:
        put(3 * third, rest, src[pl.ds(rows(at + 2 * third), rest), :])


def table_tile(start):
    v = start & 2147483647
    v = v ^ (v >> 15)
    v = (v * 277803737) & 2147483647
    v = v ^ (v >> 13)
    v = v * 1103515245
    v = v ^ (v >> 16)
    high = (v >> 5).astype(jnp.int8) & jnp.int8(31)
    low = v.astype(jnp.int8) & jnp.int8(31)
    return high.astype(jnp.bfloat16), low.astype(jnp.bfloat16)


def aggregate_kernel(
    clients,
    length,
    alive_ref,
    seeds_ref,
    quant_hbm,
    masks_hbm,
    agg_out,
    own_out,
    diff_out,
    quant,
    masked,
    base,
    partner,
    swap_from,
    swap_to,
    sent,
    arrived,
    gathered,
    own_parts,
    diff_parts,
    load_sem,
    swap_send,
    swap_recv,
    rs_send,
    rs_recv,
    ag_send,
    ag_recv,
    out_sem,
    own_send,
    own_recv,
    diff_send,
    diff_recv,
):
    rows = quant.shape[0]
    checks = seeds_ref.shape[0]
    bits = clients.bit_length() - 1
    me = lax.axis_index("clients")
    shards = lax.axis_size("shard")
    here = lax.axis_index("shard")
    start = here * length
    alive = alive_ref[0]
    stream = rows // STREAMS
    block = stream // clients
    unit = min(64, block)
    group = min(32, unit)
    per_block = block // unit
    others = clients // 2 - 1
    blocks = STREAMS * (others + 1)
    swap_rows = packed_rows(block)
    counts = [stream >> (i + 1) for i in range(bits)]
    sizes = [packed_rows(c) for c in counts]
    offsets = [sum(sizes[:i]) for i in range(bits)]
    per_stream = sum(sizes)

    barrier = pltpu.get_barrier_semaphore()
    for n in range(1, clients):
        pl.semaphore_signal(barrier, inc=1, device_id={"clients": me ^ n})
    for n in range(1, shards):
        there = lax.rem(here + n, shards)
        pl.semaphore_signal(barrier, inc=1, device_id={"shard": there})
        pl.semaphore_signal(barrier, inc=1, device_id={"shard": there, "clients": me ^ 1})
    peers = clients + 2 * shards - 3

    loads = []
    for h in range(STREAMS):
        at = pl.ds(h * stream, stream)
        loads.append(
            (
                pltpu.make_async_copy(quant_hbm.at[at], quant.at[at], load_sem.at[0, h]),
                pltpu.make_async_copy(masks_hbm.at[at], masked.at[at], load_sem.at[1, h]),
            )
        )
    for pair in loads:
        for copy in pair:
            copy.start()

    bit = [(me >> b) & 1 for b in range(bits)]
    share_even = sum(bit[i] << (bits - 1 - i) for i in range(bits))
    share_odd = sum(bit[(i + 1) % bits] << (bits - 1 - i) for i in range(bits))

    def share_of(h):
        return jnp.where(h % 2 == 1, share_odd, share_even)

    def partner_at(h, i):
        return me ^ jnp.where(h % 2 == 1, 1 << ((i + 1) % bits), 1 << i)

    def keep_row(h, i, flip=0):
        s = ((share_of(h) >> (bits - 1 - i)) ^ flip) << (bits - 1 - i)
        return pl.multiple_of(h * stream + s * block, 8)

    def block_row(w, flip=False):
        shared = w >= STREAMS * others
        h = w % STREAMS
        k = jnp.where(shared, 0, others - w // STREAMS)
        odd = h % 2 == 1
        k = jnp.where(odd, 2 * k, k)
        s = share_of(h) ^ k
        if flip:
            s = s ^ jnp.where(odd, 1, clients // 2)
        return pl.multiple_of(h * stream + s * block, 8)

    def swap_copy(w):
        at = pl.ds(pl.multiple_of(w * swap_rows, 8), swap_rows)
        return pltpu.make_async_remote_copy(
            src_ref=swap_from.at[at],
            dst_ref=swap_to.at[at],
            send_sem=swap_send.at[w],
            recv_sem=swap_recv.at[w],
            device_id={"clients": me ^ 1},
        )

    def rs_at(h, i):
        return pl.multiple_of(h * per_stream + offsets[i], 8)

    def rs_copy(h, i):
        at = pl.ds(rs_at(h, i), sizes[i])
        return pltpu.make_async_remote_copy(
            src_ref=sent.at[at],
            dst_ref=arrived.at[at],
            send_sem=rs_send.at[h, i],
            recv_sem=rs_recv.at[h, i],
            device_id={"clients": partner_at(h, i)},
        )

    def rs_pack(h, i):
        pack_block(masked, keep_row(h, i, 1), sent, rs_at(h, i), counts[i])

    def rs_take(h, i):
        rs_copy(h, i).wait()
        keep = keep_row(h, i)

        def put(at, n, v):
            spot = pl.ds(pl.multiple_of(keep + at, 8), n)
            masked[spot, :] = wrap_once(masked[spot, :] + v)

        unpack_block(arrived, rs_at(h, i), counts[i], put)

    def ag_slice(h, j, flip):
        s = ((share_of(h) >> j) ^ flip) << j
        at = pl.multiple_of((h * clients + s) * swap_rows, 8)
        return gathered.at[pl.ds(at, swap_rows << j)]

    def ag_copy(h, j, flip=0):
        return pltpu.make_async_remote_copy(
            src_ref=ag_slice(h, j, flip),
            dst_ref=ag_slice(h, j, flip),
            send_sem=ag_send.at[h, j],
            recv_sem=ag_recv.at[h, j],
            device_id={"clients": partner_at(h, bits - 1 - j)},
        )

    def store_copy(h):
        at = pl.ds(pl.multiple_of(h * clients * swap_rows, 8), clients * swap_rows)
        return pltpu.make_async_copy(gathered.at[at], agg_out.at[at], out_sem.at[h])

    lane = lax.broadcasted_iota(jnp.int32, (8, LANES), 1)
    sub = lax.broadcasted_iota(jnp.int32, (8, LANES), 0)
    lane = (lane + start) * 747796405
    for g in range(checks // 8):
        tile = lane
        for r in range(8):
            tile = tile + jnp.where(sub == r, seeds_ref[8 * g + r], 0)
        base[pl.ds(8 * g, 8), :] = tile

    step = min(64, stream)
    for h, pair in enumerate(loads):
        for copy in pair:
            copy.wait()

        @pl.loop(0, stream // step)
        def _(i, h=h):
            at = pl.ds(pl.multiple_of(h * stream + i * step, 8), step)
            s = wrap_once(wrap_once(quant[at, :] + masked[at, :]))
            masked[at, :] = s * alive

        rs_pack(h, 0)

    @pl.loop(0, blocks)
    def _(w):
        pack_block(quant, block_row(w, True), swap_from, w * swap_rows, block)

    pl.semaphore_wait(barrier, peers)
    swap_copy(0).start()
    for h in range(STREAMS):
        rs_copy(h, 0).start()
        if h == 0:
            for w in range(1, AHEAD):
                swap_copy(w).start()

    empty = jnp.zeros((8, LANES), jnp.float32)
    shift = 7 * (sub & 3)
    second = sub >= 4

    def work(u, total, share):
        w = u // per_block

        @pl.when(u % per_block == 0)
        def _():
            swap_copy(w).wait()

            @pl.when(w + AHEAD < blocks)
            def _():
                swap_copy(w + AHEAD).start()

            def put(at, n, v):
                partner[pl.ds(pl.multiple_of(at, 8), n), :] = v

            unpack_block(swap_to, w * swap_rows, block, put)

        inner = (u % per_block) * unit
        row = block_row(w) + inner
        for g in range(unit // group):
            highs, lows, pieces = [], [], []
            for k in range(g * group, (g + 1) * group):
                at = row + k
                high, low = table_tile(base[...] + at * STRIDE)
                highs.append(high)
                lows.append(low)
                one = jnp.broadcast_to(quant[pl.ds(at, 1), :], (8, LANES))
                two = jnp.broadcast_to(partner[pl.ds(inner + k, 1), :], (8, LANES))
                both = ((jnp.where(second, two, one) >> shift) & 127).astype(jnp.float32)
                third = empty
                if share:
                    three = jnp.broadcast_to(masked[pl.ds(at, 1), :], (8, LANES))
                    third = jnp.where(second, 0, (three >> shift) & 127).astype(jnp.float32)
                pieces.append(jnp.concatenate([both, third], 0).astype(jnp.bfloat16))
            table = jnp.concatenate([jnp.concatenate(highs, 1), jnp.concatenate(lows, 1)], 0)
            part = lax.dot_general(
                jnp.concatenate(pieces, 1),
                table,
                (((1,), (1,)), ((), ())),
                preferred_element_type=jnp.float32,
            )
            total = reduce_mod(total + part.astype(jnp.int32))
        return total

    units = blocks * per_block
    plain = STREAMS * others * per_block
    actions = bits * STREAMS
    early = units // 2
    first = min(3, early)

    def rs_stop(a):
        return first + (early - first) * a // actions

    def ag_stop(a):
        return early + (units - early) * (a + 1) // actions

    def compute(lo, hi, total, kinds):
        if "plain" in kinds:
            total = lax.fori_loop(
                lo, jnp.minimum(hi, plain), lambda u, t: work(u, t, False), total
            )
        if "share" in kinds:
            total = lax.fori_loop(
                jnp.maximum(lo, plain), hi, lambda u, t: work(u, t, True), total
            )
        return total

    total = jnp.zeros((16, LANES), jnp.int32)
    for i in range(bits):

        def turn(h, total, i=i):
            a = i * STREAMS + h
            lo = jnp.where(a == 0, 0, rs_stop(a - 1))
            total = compute(lo, rs_stop(a), total, ("plain",))
            rs_take(h, i)
            if i < bits - 1:
                rs_pack(h, i + 1)
                rs_copy(h, i + 1).start()
            else:
                spot = pl.multiple_of((h * clients + share_of(h)) * swap_rows, 8)
                pack_block(masked, keep_row(h, i), gathered, spot, block)
                ag_copy(h, 0).start()
            return total

        total = lax.fori_loop(0, STREAMS, turn, total)
    for j in range(bits):
        kinds = []
        lo_static = rs_stop(actions - 1) if j == 0 else ag_stop(j * STREAMS - 1)
        hi_static = ag_stop((j + 1) * STREAMS - 1)
        if lo_static < plain:
            kinds.append("plain")
        if hi_static > plain:
            kinds.append("share")

        def turn(h, total, j=j, kinds=tuple(kinds)):
            a = j * STREAMS + h
            lo = jnp.where(a == 0, rs_stop(actions - 1), ag_stop(a - 1))
            total = compute(lo, ag_stop(a), total, kinds)
            ag_copy(h, j).wait_send()
            ag_copy(h, j, 1).wait_recv()
            if j < bits - 1:
                ag_copy(h, j + 1).start()
            else:
                store_copy(h).start()
            return total

        total = lax.fori_loop(0, STREAMS, turn, total)

    own_parts[0] = total
    own_copies = []
    for n in range(1, 2 * shards):
        where = {"shard": lax.rem(here + n % shards, shards)} if n % shards else {}
        if n >= shards:
            where["clients"] = me ^ 1
        own_copies.append(
            pltpu.make_async_remote_copy(
                src_ref=own_parts.at[0],
                dst_ref=own_parts.at[n],
                send_sem=own_send.at[n],
                recv_sem=own_recv.at[n],
                device_id=where,
            )
        )
    for copy in own_copies:
        copy.start()
    for copy in own_copies:
        copy.wait()
    mine, theirs = own_parts[0], own_parts[shards]
    for n in range(1, shards):
        mine = mine + own_parts[n]
        theirs = theirs + own_parts[shards + n]
    total = reduce_mod(mine[:8] + pltpu.roll(theirs[:8], 4, 0))
    own_out[...] = total
    diff = reduce_mod(mine[8:]) - total * alive
    diff = jnp.where(diff < 0, diff + modulus, diff)
    diff_parts[0] = diff
    diff_copies = [
        pltpu.make_async_remote_copy(
            src_ref=diff_parts.at[0],
            dst_ref=diff_parts.at[n],
            send_sem=diff_send.at[n],
            recv_sem=diff_recv.at[n],
            device_id={"clients": me ^ n},
        )
        for n in range(1, clients)
    ]
    for copy in diff_copies:
        copy.start()
    for copy in diff_copies:
        copy.wait()
    for n in range(1, clients):
        diff = diff + diff_parts[n]
    diff_out[...] = reduce_mod(diff)
    for h in range(STREAMS):
        store_copy(h).wait()


def aggregate_and_project(quantized, pair_masks, alive_flags, row_seeds, clients, shards):
    length = quantized.shape[1]
    rows = length // LANES
    checks = row_seeds.shape[0]
    bits = clients.bit_length() - 1
    block = rows // STREAMS // clients
    blocks = STREAMS * clients // 2
    swap_rows = packed_rows(block)
    half_rows = STREAMS * sum(packed_rows(rows // STREAMS >> (i + 1)) for i in range(bits))
    gather_rows = STREAMS * clients * swap_rows
    vmem = pl.BlockSpec(memory_space=pltpu.VMEM)
    smem = pl.BlockSpec(memory_space=pltpu.SMEM)
    hbm = pl.BlockSpec(memory_space=pl.ANY)
    dma = pltpu.SemaphoreType.DMA
    return pl.pallas_call(
        functools.partial(aggregate_kernel, clients, length),
        in_specs=[smem, smem, hbm, hbm],
        out_specs=[hbm, vmem, vmem],
        out_shape=[
            jax.ShapeDtypeStruct((gather_rows, LANES), jnp.int32),
            jax.ShapeDtypeStruct((8, 2 * checks), jnp.int32),
            jax.ShapeDtypeStruct((8, 2 * checks), jnp.int32),
        ],
        scratch_shapes=[
            pltpu.VMEM((rows, LANES), jnp.int32),
            pltpu.VMEM((rows, LANES), jnp.int32),
            pltpu.VMEM((checks, LANES), jnp.int32),
            pltpu.VMEM((block, LANES), jnp.int32),
            pltpu.VMEM((blocks * swap_rows, LANES), jnp.int32),
            pltpu.VMEM((blocks * swap_rows, LANES), jnp.int32),
            pltpu.VMEM((half_rows, LANES), jnp.int32),
            pltpu.VMEM((half_rows, LANES), jnp.int32),
            pltpu.VMEM((gather_rows, LANES), jnp.int32),
            pltpu.VMEM((2 * shards, 16, 2 * checks), jnp.int32),
            pltpu.VMEM((clients, 8, 2 * checks), jnp.int32),
            dma((2, STREAMS)),
            dma((blocks,)),
            dma((blocks,)),
            dma((STREAMS, bits)),
            dma((STREAMS, bits)),
            dma((STREAMS, bits)),
            dma((STREAMS, bits)),
            dma((STREAMS,)),
            dma((2 * shards,)),
            dma((2 * shards,)),
            dma((clients,)),
            dma((clients,)),
        ],
        compiler_params=pltpu.CompilerParams(collective_id=0, has_side_effects=True),
        name="aggregate_and_project",
    )(
        alive_flags,
        row_seeds,
        quantized.reshape(rows, LANES),
        pair_masks.reshape(rows, LANES),
    )


def checksum(parts):
    checks = parts.shape[1] // 2
    parts = reduce_mod(parts[:, :checks] * 32 + parts[:, checks:])
    return reduce_mod(reduce_mod(parts[2:3] * 128 + parts[1:2]) * 128 + parts[0:1])


def finish_kernel(clients, packed, own, diff, agg_out, own_out, diff_out):
    block = agg_out.shape[0] // clients
    swap_rows = packed_rows(block)
    for n in range(clients):

        def put(at, count, v, n=n):
            agg_out[pl.ds(pl.multiple_of(n * block + at, 8), count), :] = v

        unpack_block(packed, n * swap_rows, block, put)
    own_out[...] = checksum(own[...])
    diff_out[...] = checksum(diff[...])


def finish(packed, own, diff, rows, clients):
    checks = own.shape[1] // 2
    small = pl.BlockSpec((8, 2 * checks), lambda i: (0, 0))
    result = pl.BlockSpec((1, checks), lambda i: (0, 0))
    return pl.pallas_call(
        functools.partial(finish_kernel, clients),
        grid=(STREAMS,),
        in_specs=[
            pl.BlockSpec((packed.shape[0] // STREAMS, LANES), lambda i: (i, 0)),
            small,
            small,
        ],
        out_specs=[pl.BlockSpec((rows // STREAMS, LANES), lambda i: (i, 0)), result, result],
        out_shape=[
            jax.ShapeDtypeStruct((rows, LANES), jnp.int32),
            jax.ShapeDtypeStruct((1, checks), jnp.int32),
            jax.ShapeDtypeStruct((1, checks), jnp.int32),
        ],
        name="finish",
    )(packed, own, diff)


def body(quantized, pair_masks, alive_flags, row_seeds):
    length = quantized.shape[1]
    clients = lax.axis_size("clients")
    shards = lax.axis_size("shard")
    packed, own, diff = aggregate_and_project(
        quantized, pair_masks, alive_flags, row_seeds, clients, shards
    )
    aggregate, own, diff = finish(packed, own, diff, length // LANES, clients)
    return (aggregate.reshape(length), own, diff.reshape(-1))


def solution(mesh):
    placed = (P("clients", "shard"), P("clients", "shard"), P("clients"), P())
    return jax.shard_map(
        body,
        mesh=mesh,
        in_specs=placed,
        out_specs=(P("shard"), P("clients", None), P()),
        check_vma=False,
    )
```

```python
import functools

import jax
import jax.numpy as jnp
from jax import lax
from jax.experimental import pallas as pl
from jax.experimental.pallas import tpu as pltpu
from jax.sharding import PartitionSpec as P

modulus = 2097143
mask21 = 2097151
LANES = 128
STREAMS = 4
AHEAD = 3
STRIDE = (LANES * 747796405 + 2147483648) % 4294967296 - 2147483648


def reduce_mod(x):
    x = (x & mask21) + (x >> 21) * 9
    return jnp.where(x >= modulus, x - modulus, x)


def wrap_once(x):
    return jnp.where(x >= modulus, x - modulus, x)


def packed_rows(count):
    tiles = count // 8
    return 8 * (2 * (tiles // 3) + tiles % 3)


def pack3(a, b, c):
    return a | (c << 21), b | ((c >> 11) << 21)


def unpack3(x, y):
    c = lax.shift_right_logical(x, 21) | ((y >> 21) << 11)
    return x & mask21, y & mask21, c


def each_step(tiles, fn):
    step = max(d for d in range(1, 9) if tiles % d == 0)

    def one(i):
        fn(i * step * 8, step * 8)

    if tiles == step:
        one(0)
    else:
        pl.loop(0, tiles // step)(one)


def pack_block(src, start, dst, at, count):
    third = 8 * (count // 24)
    rest = count - 3 * third

    def rows(x):
        return pl.multiple_of(x, 8)

    if third:

        def one(i, n):
            a = src[pl.ds(rows(start + i), n), :]
            b = src[pl.ds(rows(start + third + i), n), :]
            c = src[pl.ds(rows(start + 2 * third + i), n), :]
            x, y = pack3(a, b, c)
            dst[pl.ds(rows(at + i), n), :] = x
            dst[pl.ds(rows(at + third + i), n), :] = y

        each_step(third // 8, one)
    if rest:
        dst[pl.ds(rows(at + 2 * third), rest), :] = src[pl.ds(rows(start + 3 * third), rest), :]


def unpack_block(src, at, count, put):
    third = 8 * (count // 24)
    rest = count - 3 * third

    def rows(x):
        return pl.multiple_of(x, 8)

    if third:

        def one(i, n):
            x = src[pl.ds(rows(at + i), n), :]
            y = src[pl.ds(rows(at + third + i), n), :]
            for j, v in enumerate(unpack3(x, y)):
                put(j * third + i, n, v)

        each_step(third // 8, one)
    if rest:
        put(3 * third, rest, src[pl.ds(rows(at + 2 * third), rest), :])


def table_tile(start):
    v = start & 2147483647
    v = v ^ (v >> 15)
    v = (v * 277803737) & 2147483647
    v = v ^ (v >> 13)
    v = v * 1103515245
    v = v ^ (v >> 16)
    high = (v >> 5).astype(jnp.int8) & jnp.int8(31)
    low = v.astype(jnp.int8) & jnp.int8(31)
    return high.astype(jnp.bfloat16), low.astype(jnp.bfloat16)


def aggregate_kernel(
    clients,
    length,
    alive_ref,
    seeds_ref,
    quant_hbm,
    masks_hbm,
    gathered,
    own_out,
    diff_out,
    quant,
    masked,
    base,
    partner,
    swap_from,
    swap_to,
    sent,
    arrived,
    own_parts,
    diff_parts,
    flags,
    load_sem,
    swap_send,
    swap_recv,
    rs_send,
    rs_recv,
    ag_send,
    ag_recv,
    flag_sem,
    own_send,
    own_recv,
    diff_send,
    diff_recv,
):
    rows = quant.shape[0]
    checks = seeds_ref.shape[0]
    bits = clients.bit_length() - 1
    me = lax.axis_index("clients")
    shards = lax.axis_size("shard")
    here = lax.axis_index("shard")
    start = here * length
    alive = alive_ref[0]
    stream = rows // STREAMS
    block = stream // clients
    unit = min(64, block)
    group = min(32, unit)
    per_block = block // unit
    others = clients // 2 - 1
    blocks = STREAMS * (others + 1)
    swap_rows = packed_rows(block)
    counts = [stream >> (i + 1) for i in range(bits)]
    sizes = [packed_rows(c) for c in counts]
    offsets = [sum(sizes[:i]) for i in range(bits)]
    per_stream = sum(sizes)

    barrier = pltpu.get_barrier_semaphore()
    for b in range(bits):
        pl.semaphore_signal(barrier, inc=1, device_id={"clients": me ^ (1 << b)})
    for n in range(1, shards):
        pl.semaphore_signal(barrier, inc=1, device_id={"shard": lax.rem(here + n, shards)})
    peers = bits + shards - 1

    loads = []
    for h in range(STREAMS):
        at = pl.ds(h * stream, stream)
        loads.append(
            (
                pltpu.make_async_copy(quant_hbm.at[at], quant.at[at], load_sem.at[0, h]),
                pltpu.make_async_copy(masks_hbm.at[at], masked.at[at], load_sem.at[1, h]),
            )
        )
    for pair in loads:
        for copy in pair:
            copy.start()

    bit = [(me >> b) & 1 for b in range(bits)]
    share_even = sum(bit[i] << (bits - 1 - i) for i in range(bits))
    share_odd = sum(bit[(i + 1) % bits] << (bits - 1 - i) for i in range(bits))

    def share_of(h):
        return jnp.where(h % 2 == 1, share_odd, share_even)

    def partner_at(h, i):
        return me ^ jnp.where(h % 2 == 1, 1 << ((i + 1) % bits), 1 << i)

    def keep_row(h, i, flip=0):
        s = ((share_of(h) >> (bits - 1 - i)) ^ flip) << (bits - 1 - i)
        return pl.multiple_of(h * stream + s * block, 8)

    def block_row(w, flip=False):
        shared = w >= STREAMS * others
        h = w % STREAMS
        k = jnp.where(shared, 0, others - w // STREAMS)
        odd = h % 2 == 1
        k = jnp.where(odd, 2 * k, k)
        s = share_of(h) ^ k
        if flip:
            s = s ^ jnp.where(odd, 1, clients // 2)
        return pl.multiple_of(h * stream + s * block, 8)

    def swap_copy(w):
        at = pl.ds(pl.multiple_of(w * swap_rows, 8), swap_rows)
        return pltpu.make_async_remote_copy(
            src_ref=swap_from.at[at],
            dst_ref=swap_to.at[at],
            send_sem=swap_send.at[w],
            recv_sem=swap_recv.at[w],
            device_id={"clients": me ^ 1},
        )

    def rs_at(h, i):
        return pl.multiple_of(h * per_stream + offsets[i], 8)

    def rs_copy(h, i):
        at = pl.ds(rs_at(h, i), sizes[i])
        return pltpu.make_async_remote_copy(
            src_ref=sent.at[at],
            dst_ref=arrived.at[at],
            send_sem=rs_send.at[h, i],
            recv_sem=rs_recv.at[h, i],
            device_id={"clients": partner_at(h, i)},
        )

    def rs_pack(h, i):
        pack_block(masked, keep_row(h, i, 1), sent, rs_at(h, i), counts[i])

    def rs_take(h, i):
        rs_copy(h, i).wait()
        keep = keep_row(h, i)

        def put(at, n, v):
            spot = pl.ds(pl.multiple_of(keep + at, 8), n)
            masked[spot, :] = wrap_once(masked[spot, :] + v)

        unpack_block(arrived, rs_at(h, i), counts[i], put)

    def ag_slice(h, j, flip):
        s = ((share_of(h) >> j) ^ flip) << j
        at = pl.multiple_of((h * clients + s) * swap_rows, 8)
        return gathered.at[pl.ds(at, swap_rows << j)]

    def ag_copy(h, j, flip=0):
        return pltpu.make_async_remote_copy(
            src_ref=ag_slice(h, j, flip),
            dst_ref=ag_slice(h, j, flip),
            send_sem=ag_send.at[h, j],
            recv_sem=ag_recv.at[h, j],
            device_id={"clients": partner_at(h, bits - 1 - j)},
        )

    lane = lax.broadcasted_iota(jnp.int32, (8, LANES), 1)
    sub = lax.broadcasted_iota(jnp.int32, (8, LANES), 0)
    lane = (lane + start) * 747796405
    for g in range(checks // 8):
        tile = lane
        for r in range(8):
            tile = tile + jnp.where(sub == r, seeds_ref[8 * g + r], 0)
        base[pl.ds(8 * g, 8), :] = tile

    step = min(64, stream)
    for h, pair in enumerate(loads):
        for copy in pair:
            copy.wait()

        @pl.loop(0, stream // step)
        def _(i, h=h):
            at = pl.ds(pl.multiple_of(h * stream + i * step, 8), step)
            s = wrap_once(wrap_once(quant[at, :] + masked[at, :]))
            masked[at, :] = s * alive

        rs_pack(h, 0)

    @pl.loop(0, blocks)
    def _(w):
        pack_block(quant, block_row(w, True), swap_from, w * swap_rows, block)

    flags[0] = jnp.full((8, LANES), alive)
    flag_copy = pltpu.make_async_remote_copy(
        src_ref=flags.at[0],
        dst_ref=flags.at[1],
        send_sem=flag_sem.at[0],
        recv_sem=flag_sem.at[1],
        device_id={"clients": me ^ 1},
    )

    pl.semaphore_wait(barrier, peers)
    swap_copy(0).start()
    flag_copy.start()
    for h in range(STREAMS):
        rs_copy(h, 0).start()
        if h == 0:
            for w in range(1, AHEAD):
                swap_copy(w).start()

    empty = jnp.zeros((8, LANES), jnp.float32)
    shift = 7 * (sub & 3)
    second = sub >= 4

    def work(u, total, share):
        w = u // per_block

        @pl.when(u % per_block == 0)
        def _():
            swap_copy(w).wait()

            @pl.when(w + AHEAD < blocks)
            def _():
                swap_copy(w + AHEAD).start()

            def put(at, n, v):
                partner[pl.ds(pl.multiple_of(at, 8), n), :] = v

            unpack_block(swap_to, w * swap_rows, block, put)

        inner = (u % per_block) * unit
        row = block_row(w) + inner
        for g in range(unit // group):
            highs, lows, pieces = [], [], []
            for k in range(g * group, (g + 1) * group):
                at = row + k
                high, low = table_tile(base[...] + at * STRIDE)
                highs.append(high)
                lows.append(low)
                one = jnp.broadcast_to(quant[pl.ds(at, 1), :], (8, LANES))
                two = jnp.broadcast_to(partner[pl.ds(inner + k, 1), :], (8, LANES))
                both = ((jnp.where(second, two, one) >> shift) & 127).astype(jnp.float32)
                third = empty
                if share:
                    three = jnp.broadcast_to(masked[pl.ds(at, 1), :], (8, LANES))
                    third = jnp.where(second, 0, (three >> shift) & 127).astype(jnp.float32)
                pieces.append(jnp.concatenate([both, third], 0).astype(jnp.bfloat16))
            table = jnp.concatenate([jnp.concatenate(highs, 1), jnp.concatenate(lows, 1)], 0)
            part = lax.dot_general(
                jnp.concatenate(pieces, 1),
                table,
                (((1,), (1,)), ((), ())),
                preferred_element_type=jnp.float32,
            )
            total = reduce_mod(total + part.astype(jnp.int32))
        return total

    units = blocks * per_block
    plain = STREAMS * others * per_block
    actions = bits * STREAMS
    early = units // 2
    first = min(3, early)

    def rs_stop(a):
        return first + (early - first) * a // actions

    def ag_stop(a):
        return early + (units - early) * (a + 1) // actions

    def compute(lo, hi, total, kinds):
        if "plain" in kinds:
            total = lax.fori_loop(
                lo, jnp.minimum(hi, plain), lambda u, t: work(u, t, False), total
            )
        if "share" in kinds:
            total = lax.fori_loop(
                jnp.maximum(lo, plain), hi, lambda u, t: work(u, t, True), total
            )
        return total

    total = jnp.zeros((16, LANES), jnp.int32)
    for i in range(bits):

        def turn(h, total, i=i):
            a = i * STREAMS + h
            lo = jnp.where(a == 0, 0, rs_stop(a - 1))
            total = compute(lo, rs_stop(a), total, ("plain",))
            rs_take(h, i)
            if i < bits - 1:
                rs_pack(h, i + 1)
                rs_copy(h, i + 1).start()
            else:
                spot = pl.multiple_of((h * clients + share_of(h)) * swap_rows, 8)
                pack_block(masked, keep_row(h, i), gathered, spot, block)
                ag_copy(h, 0).start()
            return total

        total = lax.fori_loop(0, STREAMS, turn, total)
    for j in range(bits):
        kinds = []
        lo_static = rs_stop(actions - 1) if j == 0 else ag_stop(j * STREAMS - 1)
        hi_static = ag_stop((j + 1) * STREAMS - 1)
        if lo_static < plain:
            kinds.append("plain")
        if hi_static > plain:
            kinds.append("share")

        def turn(h, total, j=j, kinds=tuple(kinds)):
            a = j * STREAMS + h
            lo = jnp.where(a == 0, rs_stop(actions - 1), ag_stop(a - 1))
            total = compute(lo, ag_stop(a), total, kinds)
            ag_copy(h, j).wait_send()
            ag_copy(h, j, 1).wait_recv()
            if j < bits - 1:
                ag_copy(h, j + 1).start()
            return total

        total = lax.fori_loop(0, STREAMS, turn, total)

    flag_copy.wait()
    own = total[:8]
    diff = total[8:] - own * alive - pltpu.roll(own, 4, 0) * flags[1]
    diff = jnp.where(diff < 0, diff + modulus, diff)
    diff = jnp.where(diff < 0, diff + modulus, diff)
    own_parts[0] = own
    diff_parts[0] = diff

    def own_copy(n):
        return pltpu.make_async_remote_copy(
            src_ref=own_parts.at[0],
            dst_ref=own_parts.at[n],
            send_sem=own_send.at[n],
            recv_sem=own_recv.at[n],
            device_id={"clients": me ^ (n // shards), "shard": (here + n) % shards},
        )

    def diff_copy(n):
        return pltpu.make_async_remote_copy(
            src_ref=diff_parts.at[0],
            dst_ref=diff_parts.at[n],
            send_sem=diff_send.at[n],
            recv_sem=diff_recv.at[n],
            device_id={"clients": me ^ (n // shards), "shard": (here + n) % shards},
        )

    @pl.loop(1, clients * shards)
    def _(n):
        diff_copy(clients * shards - n).start()

    for n in range(1, 2 * shards):
        own_copy(n).start()
    for n in range(1, 2 * shards):
        own_copy(n).wait()
    mine, theirs = own_parts[0], own_parts[shards]
    for n in range(1, shards):
        mine = mine + own_parts[n]
        theirs = theirs + own_parts[shards + n]
    own_out[...] = reduce_mod(mine + pltpu.roll(theirs, 4, 0))

    def add_diff(n, diff):
        diff_copy(n).wait()
        return diff + diff_parts[n]

    diff_out[...] = reduce_mod(lax.fori_loop(1, clients * shards, add_diff, diff))


def aggregate_and_project(quantized, pair_masks, alive_flags, row_seeds, clients, shards):
    length = quantized.shape[1]
    rows = length // LANES
    checks = row_seeds.shape[0]
    bits = clients.bit_length() - 1
    block = rows // STREAMS // clients
    blocks = STREAMS * clients // 2
    swap_rows = packed_rows(block)
    half_rows = STREAMS * sum(packed_rows(rows // STREAMS >> (i + 1)) for i in range(bits))
    gather_rows = STREAMS * clients * swap_rows
    vmem = pl.BlockSpec(memory_space=pltpu.VMEM)
    smem = pl.BlockSpec(memory_space=pltpu.SMEM)
    hbm = pl.BlockSpec(memory_space=pl.ANY)
    dma = pltpu.SemaphoreType.DMA
    return pl.pallas_call(
        functools.partial(aggregate_kernel, clients, length),
        in_specs=[smem, smem, hbm, hbm],
        out_specs=[vmem, vmem, vmem],
        out_shape=[
            pltpu.VMEM((gather_rows, LANES), jnp.int32),
            pltpu.VMEM((8, 2 * checks), jnp.int32),
            pltpu.VMEM((8, 2 * checks), jnp.int32),
        ],
        scratch_shapes=[
            pltpu.VMEM((rows, LANES), jnp.int32),
            pltpu.VMEM((rows, LANES), jnp.int32),
            pltpu.VMEM((checks, LANES), jnp.int32),
            pltpu.VMEM((block, LANES), jnp.int32),
            pltpu.VMEM((blocks * swap_rows, LANES), jnp.int32),
            pltpu.VMEM((blocks * swap_rows, LANES), jnp.int32),
            pltpu.VMEM((half_rows, LANES), jnp.int32),
            pltpu.VMEM((half_rows, LANES), jnp.int32),
            pltpu.VMEM((2 * shards, 8, 2 * checks), jnp.int32),
            pltpu.VMEM((clients * shards, 8, 2 * checks), jnp.int32),
            pltpu.VMEM((2, 8, LANES), jnp.int32),
            dma((2, STREAMS)),
            dma((blocks,)),
            dma((blocks,)),
            dma((STREAMS, bits)),
            dma((STREAMS, bits)),
            dma((STREAMS, bits)),
            dma((STREAMS, bits)),
            dma((2,)),
            dma((2 * shards,)),
            dma((2 * shards,)),
            dma((clients * shards,)),
            dma((clients * shards,)),
        ],
        compiler_params=pltpu.CompilerParams(collective_id=0, has_side_effects=True),
        name="aggregate_and_project",
    )(
        alive_flags,
        row_seeds,
        quantized.reshape(rows, LANES),
        pair_masks.reshape(rows, LANES),
    )


def checksum(parts):
    checks = parts.shape[1] // 2
    parts = reduce_mod(parts[:, :checks] * 32 + parts[:, checks:])
    return reduce_mod(reduce_mod(parts[2:3] * 128 + parts[1:2]) * 128 + parts[0:1])


def finish_kernel(clients, packed, own, diff, agg_out, own_out, diff_out):
    block = agg_out.shape[0] // clients
    swap_rows = packed_rows(block)
    first = pl.program_id(0) * clients

    @pl.loop(0, clients)
    def _(n):
        def put(at, count, v):
            agg_out[pl.ds(pl.multiple_of(n * block + at, 8), count), :] = v

        unpack_block(packed, (first + n) * swap_rows, block, put)

    own_out[...] = checksum(own[...])
    diff_out[...] = checksum(diff[...])


def finish(packed, own, diff, rows, clients):
    checks = own.shape[1] // 2
    vmem = pl.BlockSpec(memory_space=pltpu.VMEM)
    return pl.pallas_call(
        functools.partial(finish_kernel, clients),
        grid=(STREAMS,),
        in_specs=[vmem, vmem, vmem],
        out_specs=[pl.BlockSpec((rows // STREAMS, LANES), lambda i: (i, 0)), vmem, vmem],
        out_shape=[
            jax.ShapeDtypeStruct((rows, LANES), jnp.int32),
            jax.ShapeDtypeStruct((1, checks), jnp.int32),
            jax.ShapeDtypeStruct((1, checks), jnp.int32),
        ],
        compiler_params=pltpu.CompilerParams(vmem_limit_bytes=16 * 1024 * 1024),
        name="finish",
    )(packed, own, diff)


def body(quantized, pair_masks, alive_flags, row_seeds):
    length = quantized.shape[1]
    clients = lax.axis_size("clients")
    shards = lax.axis_size("shard")
    packed, own, diff = aggregate_and_project(
        quantized, pair_masks, alive_flags, row_seeds, clients, shards
    )
    aggregate, own, diff = finish(packed, own, diff, length // LANES, clients)
    return (aggregate.reshape(length), own, diff.reshape(-1))


def solution(mesh):
    placed = (P("clients", "shard"), P("clients", "shard"), P("clients"), P())
    return jax.shard_map(
        body,
        mesh=mesh,
        in_specs=placed,
        out_specs=(P("shard"), P("clients", None), P()),
        check_vma=False,
    )
```

```python
import functools

import jax
import jax.numpy as jnp
from jax import lax
from jax.experimental import pallas as pl
from jax.experimental.pallas import tpu as pltpu
from jax.sharding import PartitionSpec as P

modulus = 2097143
mask21 = 2097151
LANES = 128
STREAMS = 4
AHEAD = 3
STRIDE = (LANES * 747796405 + 2147483648) % 4294967296 - 2147483648


def reduce_mod(x):
    x = (x & mask21) + (x >> 21) * 9
    return jnp.where(x >= modulus, x - modulus, x)


def wrap_once(x):
    return jnp.where(x >= modulus, x - modulus, x)


def packed_rows(count):
    tiles = count // 8
    return 8 * (2 * (tiles // 3) + tiles % 3)


def pack3(a, b, c):
    return a | (c << 21), b | ((c >> 11) << 21)


def unpack3(x, y):
    c = lax.shift_right_logical(x, 21) | ((y >> 21) << 11)
    return x & mask21, y & mask21, c


def each_step(tiles, fn):
    step = max(d for d in range(1, 9) if tiles % d == 0)

    def one(i):
        fn(i * step * 8, step * 8)

    if tiles == step:
        one(0)
    else:
        pl.loop(0, tiles // step)(one)


def pack_block(src, start, dst, at, count):
    third = 8 * (count // 24)
    rest = count - 3 * third

    def rows(x):
        return pl.multiple_of(x, 8)

    if third:

        def one(i, n):
            a = src[pl.ds(rows(start + i), n), :]
            b = src[pl.ds(rows(start + third + i), n), :]
            c = src[pl.ds(rows(start + 2 * third + i), n), :]
            x, y = pack3(a, b, c)
            dst[pl.ds(rows(at + i), n), :] = x
            dst[pl.ds(rows(at + third + i), n), :] = y

        each_step(third // 8, one)
    if rest:
        dst[pl.ds(rows(at + 2 * third), rest), :] = src[pl.ds(rows(start + 3 * third), rest), :]


def unpack_block(src, at, count, put):
    third = 8 * (count // 24)
    rest = count - 3 * third

    def rows(x):
        return pl.multiple_of(x, 8)

    if third:

        def one(i, n):
            x = src[pl.ds(rows(at + i), n), :]
            y = src[pl.ds(rows(at + third + i), n), :]
            for j, v in enumerate(unpack3(x, y)):
                put(j * third + i, n, v)

        each_step(third // 8, one)
    if rest:
        put(3 * third, rest, src[pl.ds(rows(at + 2 * third), rest), :])


def table_tile(start):
    v = start & 2147483647
    v = v ^ (v >> 15)
    v = (v * 277803737) & 2147483647
    v = v ^ (v >> 13)
    v = v * 1103515245
    v = v ^ (v >> 16)
    high = (v >> 5).astype(jnp.int8) & jnp.int8(31)
    low = v.astype(jnp.int8) & jnp.int8(31)
    return high.astype(jnp.bfloat16), low.astype(jnp.bfloat16)


def aggregate_kernel(
    clients,
    length,
    alive_ref,
    seeds_ref,
    quant_hbm,
    masks_hbm,
    gathered,
    sums_out,
    quant,
    masked,
    base,
    partner,
    swap_from,
    swap_to,
    sent,
    arrived,
    rows_out,
    rows_in,
    flags,
    load_sem,
    swap_send,
    swap_recv,
    rs_send,
    rs_recv,
    ag_send,
    ag_recv,
    flag_sem,
    sums_sem,
):
    rows = quant.shape[0]
    checks = seeds_ref.shape[0]
    devices = rows_in.shape[0]
    bits = clients.bit_length() - 1
    me = lax.axis_index("clients")
    shards = lax.axis_size("shard")
    here = lax.axis_index("shard")
    start = here * length
    alive = alive_ref[0]
    stream = rows // STREAMS
    block = stream // clients
    unit = min(64, block)
    group = min(32, unit)
    per_block = block // unit
    others = clients // 2 - 1
    blocks = STREAMS * (others + 1)
    swap_rows = packed_rows(block)
    counts = [stream >> (i + 1) for i in range(bits)]
    sizes = [packed_rows(c) for c in counts]
    offsets = [sum(sizes[:i]) for i in range(bits)]
    per_stream = sum(sizes)

    barrier = pltpu.get_barrier_semaphore()
    for b in range(bits):
        pl.semaphore_signal(barrier, inc=1, device_id={"clients": me ^ (1 << b)})
    for n in range(1, shards):
        pl.semaphore_signal(barrier, inc=1, device_id={"shard": lax.rem(here + n, shards)})
    peers = bits + shards - 1

    loads = []
    for h in range(STREAMS):
        at = pl.ds(h * stream, stream)
        loads.append(
            (
                pltpu.make_async_copy(quant_hbm.at[at], quant.at[at], load_sem.at[0, h]),
                pltpu.make_async_copy(masks_hbm.at[at], masked.at[at], load_sem.at[1, h]),
            )
        )
    for pair in loads:
        for copy in pair:
            copy.start()

    bit = [(me >> b) & 1 for b in range(bits)]
    share_even = sum(bit[i] << (bits - 1 - i) for i in range(bits))
    share_odd = sum(bit[(i + 1) % bits] << (bits - 1 - i) for i in range(bits))

    def share_of(h):
        return jnp.where(h % 2 == 1, share_odd, share_even)

    def partner_at(h, i):
        return me ^ jnp.where(h % 2 == 1, 1 << ((i + 1) % bits), 1 << i)

    def keep_row(h, i, flip=0):
        s = ((share_of(h) >> (bits - 1 - i)) ^ flip) << (bits - 1 - i)
        return pl.multiple_of(h * stream + s * block, 8)

    def block_row(w, flip=False):
        shared = w >= STREAMS * others
        h = w % STREAMS
        k = jnp.where(shared, 0, others - w // STREAMS)
        odd = h % 2 == 1
        k = jnp.where(odd, 2 * k, k)
        s = share_of(h) ^ k
        if flip:
            s = s ^ jnp.where(odd, 1, clients // 2)
        return pl.multiple_of(h * stream + s * block, 8)

    def swap_copy(w):
        at = pl.ds(pl.multiple_of(w * swap_rows, 8), swap_rows)
        return pltpu.make_async_remote_copy(
            src_ref=swap_from.at[at],
            dst_ref=swap_to.at[at],
            send_sem=swap_send.at[w],
            recv_sem=swap_recv.at[w],
            device_id={"clients": me ^ 1},
        )

    def rs_at(h, i):
        return pl.multiple_of(h * per_stream + offsets[i], 8)

    def rs_copy(h, i):
        at = pl.ds(rs_at(h, i), sizes[i])
        return pltpu.make_async_remote_copy(
            src_ref=sent.at[at],
            dst_ref=arrived.at[at],
            send_sem=rs_send.at[h, i],
            recv_sem=rs_recv.at[h, i],
            device_id={"clients": partner_at(h, i)},
        )

    def rs_pack(h, i):
        pack_block(masked, keep_row(h, i, 1), sent, rs_at(h, i), counts[i])

    def rs_take(h, i):
        rs_copy(h, i).wait()
        keep = keep_row(h, i)

        def put(at, n, v):
            spot = pl.ds(pl.multiple_of(keep + at, 8), n)
            masked[spot, :] = wrap_once(masked[spot, :] + v)

        unpack_block(arrived, rs_at(h, i), counts[i], put)

    def ag_slice(h, j, flip):
        s = ((share_of(h) >> j) ^ flip) << j
        at = pl.multiple_of((h * clients + s) * swap_rows, 8)
        return gathered.at[pl.ds(at, swap_rows << j)]

    def ag_copy(h, j, flip=0):
        return pltpu.make_async_remote_copy(
            src_ref=ag_slice(h, j, flip),
            dst_ref=ag_slice(h, j, flip),
            send_sem=ag_send.at[h, j],
            recv_sem=ag_recv.at[h, j],
            device_id={"clients": partner_at(h, bits - 1 - j)},
        )

    lane = lax.broadcasted_iota(jnp.int32, (8, LANES), 1)
    sub = lax.broadcasted_iota(jnp.int32, (8, LANES), 0)
    lane = (lane + start) * 747796405
    for g in range(checks // 8):
        tile = lane
        for r in range(8):
            tile = tile + jnp.where(sub == r, seeds_ref[8 * g + r], 0)
        base[pl.ds(8 * g, 8), :] = tile

    step = min(64, stream)
    for h, pair in enumerate(loads):
        for copy in pair:
            copy.wait()

        @pl.loop(0, stream // step)
        def _(i, h=h):
            at = pl.ds(pl.multiple_of(h * stream + i * step, 8), step)
            s = wrap_once(wrap_once(quant[at, :] + masked[at, :]))
            masked[at, :] = s * alive

        rs_pack(h, 0)

    @pl.loop(0, blocks)
    def _(w):
        pack_block(quant, block_row(w, True), swap_from, w * swap_rows, block)

    flags[0] = jnp.full((8, LANES), alive)
    flag_copy = pltpu.make_async_remote_copy(
        src_ref=flags.at[0],
        dst_ref=flags.at[1],
        send_sem=flag_sem.at[0],
        recv_sem=flag_sem.at[1],
        device_id={"clients": me ^ 1},
    )

    pl.semaphore_wait(barrier, peers)
    swap_copy(0).start()
    flag_copy.start()
    for h in range(STREAMS):
        rs_copy(h, 0).start()
        if h == 0:
            for w in range(1, AHEAD):
                swap_copy(w).start()

    empty = jnp.zeros((8, LANES), jnp.float32)
    shift = 7 * (sub & 3)
    second = sub >= 4

    def work(u, total, share):
        w = u // per_block

        @pl.when(u % per_block == 0)
        def _():
            swap_copy(w).wait()

            @pl.when(w + AHEAD < blocks)
            def _():
                swap_copy(w + AHEAD).start()

            def put(at, n, v):
                partner[pl.ds(pl.multiple_of(at, 8), n), :] = v

            unpack_block(swap_to, w * swap_rows, block, put)

        inner = (u % per_block) * unit
        row = block_row(w) + inner
        for g in range(unit // group):
            highs, lows, pieces = [], [], []
            for k in range(g * group, (g + 1) * group):
                at = row + k
                high, low = table_tile(base[...] + at * STRIDE)
                highs.append(high)
                lows.append(low)
                one = jnp.broadcast_to(quant[pl.ds(at, 1), :], (8, LANES))
                two = jnp.broadcast_to(partner[pl.ds(inner + k, 1), :], (8, LANES))
                both = ((jnp.where(second, two, one) >> shift) & 127).astype(jnp.float32)
                third = empty
                if share:
                    three = jnp.broadcast_to(masked[pl.ds(at, 1), :], (8, LANES))
                    third = jnp.where(second, 0, (three >> shift) & 127).astype(jnp.float32)
                pieces.append(jnp.concatenate([both, third], 0).astype(jnp.bfloat16))
            table = jnp.concatenate([jnp.concatenate(highs, 1), jnp.concatenate(lows, 1)], 0)
            part = lax.dot_general(
                jnp.concatenate(pieces, 1),
                table,
                (((1,), (1,)), ((), ())),
                preferred_element_type=jnp.float32,
            )
            total = reduce_mod(total + part.astype(jnp.int32))
        return total

    units = blocks * per_block
    plain = STREAMS * others * per_block
    actions = bits * STREAMS
    early = units // 2
    first = min(3, early)

    def rs_stop(a):
        return first + (early - first) * a // actions

    def ag_stop(a):
        return early + (units - early) * (a + 1) // (actions - STREAMS)

    def compute(lo, hi, total, kinds):
        if "plain" in kinds:
            total = lax.fori_loop(
                lo, jnp.minimum(hi, plain), lambda u, t: work(u, t, False), total
            )
        if "share" in kinds:
            total = lax.fori_loop(
                jnp.maximum(lo, plain), hi, lambda u, t: work(u, t, True), total
            )
        return total

    total = jnp.zeros((16, LANES), jnp.int32)
    for i in range(bits):

        def turn(h, total, i=i):
            a = i * STREAMS + h
            h = h ^ 1
            lo = jnp.where(a == 0, 0, rs_stop(a - 1))
            total = compute(lo, rs_stop(a), total, ("plain",))
            rs_take(h, i)
            if i < bits - 1:
                rs_pack(h, i + 1)
                rs_copy(h, i + 1).start()
            else:
                spot = pl.multiple_of((h * clients + share_of(h)) * swap_rows, 8)
                pack_block(masked, keep_row(h, i), gathered, spot, block)
                ag_copy(h, 0).start()
            return total

        total = lax.fori_loop(0, STREAMS, turn, total)
    def gather_turn(h, j):
        ag_copy(h, j).wait_send()
        ag_copy(h, j, 1).wait_recv()
        if j < bits - 1:
            ag_copy(h, j + 1).start()

    for j in range(bits - 1):
        kinds = []
        lo_static = rs_stop(actions - 1) if j == 0 else ag_stop(j * STREAMS - 1)
        hi_static = ag_stop((j + 1) * STREAMS - 1)
        if lo_static < plain:
            kinds.append("plain")
        if hi_static > plain:
            kinds.append("share")

        def turn(h, total, j=j, kinds=tuple(kinds)):
            a = j * STREAMS + h
            h = h ^ 1
            lo = jnp.where(a == 0, rs_stop(actions - 1), ag_stop(a - 1))
            total = compute(lo, ag_stop(a), total, kinds)
            gather_turn(h, j)
            return total

        total = lax.fori_loop(0, STREAMS, turn, total)

    flag_copy.wait()
    total = reduce_mod(total * 32 + pltpu.roll(total, checks, 1))

    def combine(r):
        high = reduce_mod(total[r + 2 : r + 3] * 128 + total[r + 1 : r + 2])
        return reduce_mod(high * 128 + total[r : r + 1])

    own, other = combine(0), combine(4)
    diff = combine(8) - own * alive - other * flags[1, :1]
    diff = jnp.where(diff < 0, diff + modulus, diff)
    diff = jnp.where(diff < 0, diff + modulus, diff)
    left = lax.broadcasted_iota(jnp.int32, (1, LANES), 1) < checks
    mine = jnp.where(left, diff, pltpu.roll(own, checks, 1))
    rows_out[0] = mine
    rows_out[1] = jnp.where(left, diff, pltpu.roll(other, checks, 1))
    rows_in[0] = mine

    def row_copy(n):
        return pltpu.make_async_remote_copy(
            src_ref=rows_out.at[jnp.where(n // shards == 1, 1, 0)],
            dst_ref=rows_in.at[n],
            send_sem=sums_sem.at[0],
            recv_sem=sums_sem.at[1],
            device_id={"clients": me ^ (n // shards), "shard": (here + n) % shards},
        )

    @pl.loop(1, devices)
    def _(n):
        row_copy(devices - n).start()

    @pl.loop(0, STREAMS)
    def _(h):
        gather_turn(h ^ 1, bits - 1)

    landed = rows_in.at[pl.ds(1, devices - 1)]
    pltpu.make_async_copy(landed, landed, sums_sem.at[0]).wait()
    pltpu.make_async_copy(landed, landed, sums_sem.at[1]).wait()
    near = rows_in[0]
    for n in range(1, 2 * shards):
        near = near + rows_in[n]
    every = lax.fori_loop(2 * shards, devices, lambda n, t: t + rows_in[n], near)
    sums_out[...] = reduce_mod(jnp.where(left, every, near))


def aggregate_and_project(quantized, pair_masks, alive_flags, row_seeds, clients, shards):
    length = quantized.shape[1]
    rows = length // LANES
    checks = row_seeds.shape[0]
    bits = clients.bit_length() - 1
    block = rows // STREAMS // clients
    blocks = STREAMS * clients // 2
    swap_rows = packed_rows(block)
    half_rows = STREAMS * sum(packed_rows(rows // STREAMS >> (i + 1)) for i in range(bits))
    gather_rows = STREAMS * clients * swap_rows
    vmem = pl.BlockSpec(memory_space=pltpu.VMEM)
    smem = pl.BlockSpec(memory_space=pltpu.SMEM)
    hbm = pl.BlockSpec(memory_space=pl.ANY)
    dma = pltpu.SemaphoreType.DMA
    return pl.pallas_call(
        functools.partial(aggregate_kernel, clients, length),
        in_specs=[smem, smem, hbm, hbm],
        out_specs=[vmem, vmem],
        out_shape=[
            pltpu.VMEM((gather_rows, LANES), jnp.int32),
            pltpu.VMEM((1, 2 * checks), jnp.int32),
        ],
        scratch_shapes=[
            pltpu.VMEM((rows, LANES), jnp.int32),
            pltpu.VMEM((rows, LANES), jnp.int32),
            pltpu.VMEM((checks, LANES), jnp.int32),
            pltpu.VMEM((block, LANES), jnp.int32),
            pltpu.VMEM((blocks * swap_rows, LANES), jnp.int32),
            pltpu.VMEM((blocks * swap_rows, LANES), jnp.int32),
            pltpu.VMEM((half_rows, LANES), jnp.int32),
            pltpu.VMEM((half_rows, LANES), jnp.int32),
            pltpu.VMEM((2, 1, 2 * checks), jnp.int32),
            pltpu.VMEM((clients * shards, 1, 2 * checks), jnp.int32),
            pltpu.VMEM((2, 8, LANES), jnp.int32),
            dma((2, STREAMS)),
            dma((blocks,)),
            dma((blocks,)),
            dma((STREAMS, bits)),
            dma((STREAMS, bits)),
            dma((STREAMS, bits)),
            dma((STREAMS, bits)),
            dma((2,)),
            dma((2,)),
        ],
        compiler_params=pltpu.CompilerParams(collective_id=0, has_side_effects=True),
        name="aggregate_and_project",
    )(
        alive_flags,
        row_seeds,
        quantized.reshape(rows, LANES),
        pair_masks.reshape(rows, LANES),
    )


def finish_kernel(clients, packed, sums, agg_out, own_out, diff_out):
    block = agg_out.shape[0] // clients
    swap_rows = packed_rows(block)
    first = pl.program_id(0) * clients

    @pl.loop(0, clients)
    def _(n):
        def put(at, count, v):
            agg_out[pl.ds(pl.multiple_of(n * block + at, 8), count), :] = v

        unpack_block(packed, (first + n) * swap_rows, block, put)

    checks = own_out.shape[1]
    diff_out[...] = sums[:, :checks]
    own_out[...] = sums[:, checks:]


def finish(packed, sums, rows, clients):
    checks = sums.shape[1] // 2
    vmem = pl.BlockSpec(memory_space=pltpu.VMEM)
    return pl.pallas_call(
        functools.partial(finish_kernel, clients),
        grid=(STREAMS,),
        in_specs=[vmem, vmem],
        out_specs=[pl.BlockSpec((rows // STREAMS, LANES), lambda i: (i, 0)), vmem, vmem],
        out_shape=[
            jax.ShapeDtypeStruct((rows, LANES), jnp.int32),
            jax.ShapeDtypeStruct((1, checks), jnp.int32),
            jax.ShapeDtypeStruct((1, checks), jnp.int32),
        ],
        compiler_params=pltpu.CompilerParams(vmem_limit_bytes=16 * 1024 * 1024),
        name="finish",
    )(packed, sums)


def body(quantized, pair_masks, alive_flags, row_seeds):
    length = quantized.shape[1]
    clients = lax.axis_size("clients")
    shards = lax.axis_size("shard")
    packed, sums = aggregate_and_project(
        quantized, pair_masks, alive_flags, row_seeds, clients, shards
    )
    aggregate, own, diff = finish(packed, sums, length // LANES, clients)
    return (aggregate.reshape(length), own, diff.reshape(-1))


def solution(mesh):
    placed = (P("clients", "shard"), P("clients", "shard"), P("clients"), P())
    return jax.shard_map(
        body,
        mesh=mesh,
        in_specs=placed,
        out_specs=(P("shard"), P("clients", None), P()),
        check_vma=False,
    )
```

```python
import functools

import jax
import jax.numpy as jnp
from jax import lax
from jax.experimental import pallas as pl
from jax.experimental.pallas import tpu as pltpu
from jax.sharding import PartitionSpec as P

modulus = 2097143
mask21 = 2097151
LANES = 128
STREAMS = 4
AHEAD = 3
STRIDE = (LANES * 747796405 + 2147483648) % 4294967296 - 2147483648


def reduce_mod(x):
    x = (x & mask21) + (x >> 21) * 9
    return jnp.where(x >= modulus, x - modulus, x)


def wrap_once(x):
    return jnp.where(x >= modulus, x - modulus, x)


def packed_rows(count):
    tiles = count // 8
    return 8 * (2 * (tiles // 3) + tiles % 3)


def pack3(a, b, c):
    return a | (c << 21), b | ((c >> 11) << 21)


def unpack3(x, y):
    c = lax.shift_right_logical(x, 21) | ((y >> 21) << 11)
    return x & mask21, y & mask21, c


def each_step(tiles, fn):
    step = max(d for d in range(1, 9) if tiles % d == 0)

    def one(i):
        fn(i * step * 8, step * 8)

    if tiles == step:
        one(0)
    else:
        pl.loop(0, tiles // step)(one)


def pack_block(src, start, dst, at, count):
    third = 8 * (count // 24)
    rest = count - 3 * third

    def rows(x):
        return pl.multiple_of(x, 8)

    if third:

        def one(i, n):
            a = src[pl.ds(rows(start + i), n), :]
            b = src[pl.ds(rows(start + third + i), n), :]
            c = src[pl.ds(rows(start + 2 * third + i), n), :]
            x, y = pack3(a, b, c)
            dst[pl.ds(rows(at + i), n), :] = x
            dst[pl.ds(rows(at + third + i), n), :] = y

        each_step(third // 8, one)
    if rest:
        dst[pl.ds(rows(at + 2 * third), rest), :] = src[pl.ds(rows(start + 3 * third), rest), :]


def unpack_block(src, at, count, put):
    third = 8 * (count // 24)
    rest = count - 3 * third

    def rows(x):
        return pl.multiple_of(x, 8)

    if third:

        def one(i, n):
            x = src[pl.ds(rows(at + i), n), :]
            y = src[pl.ds(rows(at + third + i), n), :]
            for j, v in enumerate(unpack3(x, y)):
                put(j * third + i, n, v)

        each_step(third // 8, one)
    if rest:
        put(3 * third, rest, src[pl.ds(rows(at + 2 * third), rest), :])


def table_tile(start):
    v = start & 2147483647
    v = v ^ (v >> 15)
    v = (v * 277803737) & 2147483647
    v = v ^ (v >> 13)
    v = v * 1103515245
    v = v ^ (v >> 16)
    high = (v >> 5).astype(jnp.int8) & jnp.int8(31)
    low = v.astype(jnp.int8) & jnp.int8(31)
    return high.astype(jnp.bfloat16), low.astype(jnp.bfloat16)


def aggregate_kernel(
    clients,
    length,
    alive_ref,
    seeds_ref,
    quant_hbm,
    masks_hbm,
    gathered,
    sums_out,
    quant,
    masked,
    base,
    partner,
    swap_from,
    swap_to,
    sent,
    arrived,
    rows_out,
    rows_in,
    flags,
    load_sem,
    swap_send,
    swap_recv,
    rs_send,
    rs_recv,
    ag_send,
    ag_recv,
    flag_sem,
    sums_sem,
):
    rows = quant.shape[0]
    checks = seeds_ref.shape[0]
    devices = rows_in.shape[0]
    bits = clients.bit_length() - 1
    me = lax.axis_index("clients")
    shards = lax.axis_size("shard")
    here = lax.axis_index("shard")
    start = here * length
    alive = alive_ref[0]
    stream = rows // STREAMS
    block = stream // clients
    unit = min(128, block)
    group = min(32, unit)
    per_block = block // unit
    others = clients // 2 - 1
    blocks = STREAMS * (others + 1)
    swap_rows = packed_rows(block)
    counts = [stream >> (i + 1) for i in range(bits)]
    sizes = [packed_rows(c) for c in counts]
    offsets = [sum(sizes[:i]) for i in range(bits)]
    per_stream = sum(sizes)

    barrier = pltpu.get_barrier_semaphore()
    for b in range(bits):
        pl.semaphore_signal(barrier, inc=1, device_id={"clients": me ^ (1 << b)})
    for n in range(1, shards):
        pl.semaphore_signal(barrier, inc=1, device_id={"shard": lax.rem(here + n, shards)})
    peers = bits + shards - 1

    order = [h ^ 1 for h in range(STREAMS)]
    loads = []
    for h in range(STREAMS):
        at = pl.ds(h * stream, stream)
        loads.append(
            (
                pltpu.make_async_copy(quant_hbm.at[at], quant.at[at], load_sem.at[0, h]),
                pltpu.make_async_copy(masks_hbm.at[at], masked.at[at], load_sem.at[1, h]),
            )
        )
    for side in range(2):
        for h in order:
            loads[h][side].start()

    bit = [(me >> b) & 1 for b in range(bits)]
    share_even = sum(bit[i] << (bits - 1 - i) for i in range(bits))
    share_odd = sum(bit[(i + 1) % bits] << (bits - 1 - i) for i in range(bits))

    def share_of(h):
        return jnp.where(h % 2 == 1, share_odd, share_even)

    def partner_at(h, i):
        return me ^ jnp.where(h % 2 == 1, 1 << ((i + 1) % bits), 1 << i)

    def keep_row(h, i, flip=0):
        s = ((share_of(h) >> (bits - 1 - i)) ^ flip) << (bits - 1 - i)
        return pl.multiple_of(h * stream + s * block, 8)

    def block_row(w, flip=False):
        shared = w >= STREAMS * others
        h = w % STREAMS
        k = jnp.where(shared, 0, others - w // STREAMS)
        odd = h % 2 == 1
        k = jnp.where(odd, 2 * k, k)
        s = share_of(h) ^ k
        if flip:
            s = s ^ jnp.where(odd, 1, clients // 2)
        return pl.multiple_of(h * stream + s * block, 8)

    def swap_copy(w):
        at = pl.ds(pl.multiple_of(w * swap_rows, 8), swap_rows)
        return pltpu.make_async_remote_copy(
            src_ref=swap_from.at[at],
            dst_ref=swap_to.at[at],
            send_sem=swap_send.at[w],
            recv_sem=swap_recv.at[w],
            device_id={"clients": me ^ 1},
        )

    def rs_at(h, i):
        return pl.multiple_of(h * per_stream + offsets[i], 8)

    def rs_copy(h, i):
        at = pl.ds(rs_at(h, i), sizes[i])
        return pltpu.make_async_remote_copy(
            src_ref=sent.at[at],
            dst_ref=arrived.at[at],
            send_sem=rs_send.at[h, i],
            recv_sem=rs_recv.at[h, i],
            device_id={"clients": partner_at(h, i)},
        )

    def rs_pack(h, i):
        pack_block(masked, keep_row(h, i, 1), sent, rs_at(h, i), counts[i])

    def rs_take(h, i):
        rs_copy(h, i).wait()
        keep = keep_row(h, i)

        def put(at, n, v):
            spot = pl.ds(pl.multiple_of(keep + at, 8), n)
            masked[spot, :] = wrap_once(masked[spot, :] + v)

        unpack_block(arrived, rs_at(h, i), counts[i], put)

    def ag_slice(h, j, flip):
        s = ((share_of(h) >> j) ^ flip) << j
        at = pl.multiple_of((h * clients + s) * swap_rows, 8)
        return gathered.at[pl.ds(at, swap_rows << j)]

    def ag_copy(h, j, flip=0):
        return pltpu.make_async_remote_copy(
            src_ref=ag_slice(h, j, flip),
            dst_ref=ag_slice(h, j, flip),
            send_sem=ag_send.at[h, j],
            recv_sem=ag_recv.at[h, j],
            device_id={"clients": partner_at(h, bits - 1 - j)},
        )

    lane = lax.broadcasted_iota(jnp.int32, (8, LANES), 1)
    sub = lax.broadcasted_iota(jnp.int32, (8, LANES), 0)
    lane = (lane + start) * 747796405
    for g in range(checks // 8):
        tile = lane
        for r in range(8):
            tile = tile + jnp.where(sub == r, seeds_ref[8 * g + r], 0)
        base[pl.ds(8 * g, 8), :] = tile

    def swap_pack(w):
        pack_block(quant, block_row(w, True), swap_from, w * swap_rows, block)

    flags[0] = jnp.full((8, LANES), alive)
    flag_copy = pltpu.make_async_remote_copy(
        src_ref=flags.at[0],
        dst_ref=flags.at[1],
        send_sem=flag_sem.at[0],
        recv_sem=flag_sem.at[1],
        device_id={"clients": me ^ 1},
    )

    for h in order:
        loads[h][0].wait()
    pl.loop(0, AHEAD)(swap_pack)
    pl.semaphore_wait(barrier, peers)
    swap_copy(0).start()
    step = min(64, stream)
    for n, h in enumerate(order):
        loads[h][1].wait()

        @pl.loop(0, stream // step)
        def _(i, h=h):
            at = pl.ds(pl.multiple_of(h * stream + i * step, 8), step)
            s = wrap_once(wrap_once(quant[at, :] + masked[at, :]))
            masked[at, :] = s * alive

        rs_pack(h, 0)
        rs_copy(h, 0).start()
        if n == 1:
            for w in range(1, AHEAD):
                swap_copy(w).start()
    flag_copy.start()
    pl.loop(AHEAD, blocks)(swap_pack)

    empty = jnp.zeros((8, LANES), jnp.float32)
    shift = 7 * (sub & 3)
    second = sub >= 4

    def work(u, total, share):
        w = u // per_block

        @pl.when(u % per_block == 0)
        def _():
            swap_copy(w).wait()

            @pl.when(w + AHEAD < blocks)
            def _():
                swap_copy(w + AHEAD).start()

            def put(at, n, v):
                partner[pl.ds(pl.multiple_of(at, 8), n), :] = v

            unpack_block(swap_to, w * swap_rows, block, put)

        inner = (u % per_block) * unit
        row = block_row(w) + inner
        for g in range(unit // group):
            highs, lows, pieces = [], [], []
            for k in range(g * group, (g + 1) * group):
                at = row + k
                high, low = table_tile(base[...] + at * STRIDE)
                highs.append(high)
                lows.append(low)
                one = jnp.broadcast_to(quant[pl.ds(at, 1), :], (8, LANES))
                two = jnp.broadcast_to(partner[pl.ds(inner + k, 1), :], (8, LANES))
                both = ((jnp.where(second, two, one) >> shift) & 127).astype(jnp.float32)
                third = empty
                if share:
                    three = jnp.broadcast_to(masked[pl.ds(at, 1), :], (8, LANES))
                    third = jnp.where(second, 0, (three >> shift) & 127).astype(jnp.float32)
                pieces.append(jnp.concatenate([both, third], 0).astype(jnp.bfloat16))
            table = jnp.concatenate([jnp.concatenate(highs, 1), jnp.concatenate(lows, 1)], 0)
            part = lax.dot_general(
                jnp.concatenate(pieces, 1),
                table,
                (((1,), (1,)), ((), ())),
                preferred_element_type=jnp.float32,
            )
            total = reduce_mod(total + part.astype(jnp.int32))
        return total

    units = blocks * per_block
    plain = STREAMS * others * per_block
    actions = bits * STREAMS
    early = units * 9 // 16
    first = min(2, early)

    def rs_stop(a):
        return first + (early - first) * a // actions

    def ag_stop(a):
        return early + (units - early) * (a + 1) // (actions - STREAMS)

    def compute(lo, hi, total, kinds):
        if "plain" in kinds:
            total = lax.fori_loop(
                lo, jnp.minimum(hi, plain), lambda u, t: work(u, t, False), total
            )
        if "share" in kinds:
            total = lax.fori_loop(
                jnp.maximum(lo, plain), hi, lambda u, t: work(u, t, True), total
            )
        return total

    total = jnp.zeros((16, LANES), jnp.int32)
    for i in range(bits):

        def turn(h, total, i=i):
            a = i * STREAMS + h
            h = h ^ 1
            lo = jnp.where(a == 0, 0, rs_stop(a - 1))
            total = compute(lo, rs_stop(a), total, ("plain",))
            rs_take(h, i)
            if i < bits - 1:
                rs_pack(h, i + 1)
                rs_copy(h, i + 1).start()
            else:
                spot = pl.multiple_of((h * clients + share_of(h)) * swap_rows, 8)
                pack_block(masked, keep_row(h, i), gathered, spot, block)
                ag_copy(h, 0).start()
            return total

        total = lax.fori_loop(0, STREAMS, turn, total)
    def gather_turn(h, j):
        ag_copy(h, j).wait_send()
        ag_copy(h, j, 1).wait_recv()
        if j < bits - 1:
            ag_copy(h, j + 1).start()

    for j in range(bits - 1):
        kinds = []
        lo_static = rs_stop(actions - 1) if j == 0 else ag_stop(j * STREAMS - 1)
        hi_static = ag_stop((j + 1) * STREAMS - 1)
        if lo_static < plain:
            kinds.append("plain")
        if hi_static > plain:
            kinds.append("share")

        def turn(h, total, j=j, kinds=tuple(kinds)):
            a = j * STREAMS + h
            h = h ^ 1
            lo = jnp.where(a == 0, rs_stop(actions - 1), ag_stop(a - 1))
            total = compute(lo, ag_stop(a), total, kinds)
            gather_turn(h, j)
            return total

        total = lax.fori_loop(0, STREAMS, turn, total)

    flag_copy.wait()
    total = reduce_mod(total * 32 + pltpu.roll(total, checks, 1))

    def combine(r):
        high = reduce_mod(total[r + 2 : r + 3] * 128 + total[r + 1 : r + 2])
        return reduce_mod(high * 128 + total[r : r + 1])

    own, other = combine(0), combine(4)
    diff = combine(8) - own * alive - other * flags[1, :1]
    diff = jnp.where(diff < 0, diff + modulus, diff)
    diff = jnp.where(diff < 0, diff + modulus, diff)
    left = lax.broadcasted_iota(jnp.int32, (1, LANES), 1) < checks
    mine = jnp.where(left, diff, pltpu.roll(own, checks, 1))
    rows_out[0] = mine
    rows_out[1] = jnp.where(left, diff, pltpu.roll(other, checks, 1))
    rows_in[0] = mine

    def row_copy(n):
        return pltpu.make_async_remote_copy(
            src_ref=rows_out.at[jnp.where(n // shards == 1, 1, 0)],
            dst_ref=rows_in.at[n],
            send_sem=sums_sem.at[0],
            recv_sem=sums_sem.at[1],
            device_id={"clients": me ^ (n // shards), "shard": (here + n) % shards},
        )

    @pl.loop(1, devices)
    def _(n):
        row_copy(devices - n).start()

    @pl.loop(0, STREAMS)
    def _(h):
        gather_turn(h ^ 1, bits - 1)

    landed = rows_in.at[pl.ds(1, devices - 1)]
    pltpu.make_async_copy(landed, landed, sums_sem.at[0]).wait()
    pltpu.make_async_copy(landed, landed, sums_sem.at[1]).wait()
    near = rows_in[0]
    for n in range(1, 2 * shards):
        near = near + rows_in[n]
    every = lax.fori_loop(2 * shards, devices, lambda n, t: t + rows_in[n], near)
    sums_out[...] = reduce_mod(jnp.where(left, every, near))


def aggregate_and_project(quantized, pair_masks, alive_flags, row_seeds, clients, shards):
    length = quantized.shape[1]
    rows = length // LANES
    checks = row_seeds.shape[0]
    bits = clients.bit_length() - 1
    block = rows // STREAMS // clients
    blocks = STREAMS * clients // 2
    swap_rows = packed_rows(block)
    half_rows = STREAMS * sum(packed_rows(rows // STREAMS >> (i + 1)) for i in range(bits))
    gather_rows = STREAMS * clients * swap_rows
    vmem = pl.BlockSpec(memory_space=pltpu.VMEM)
    smem = pl.BlockSpec(memory_space=pltpu.SMEM)
    hbm = pl.BlockSpec(memory_space=pl.ANY)
    dma = pltpu.SemaphoreType.DMA
    return pl.pallas_call(
        functools.partial(aggregate_kernel, clients, length),
        in_specs=[smem, smem, hbm, hbm],
        out_specs=[vmem, vmem],
        out_shape=[
            pltpu.VMEM((gather_rows, LANES), jnp.int32),
            pltpu.VMEM((1, 2 * checks), jnp.int32),
        ],
        scratch_shapes=[
            pltpu.VMEM((rows, LANES), jnp.int32),
            pltpu.VMEM((rows, LANES), jnp.int32),
            pltpu.VMEM((checks, LANES), jnp.int32),
            pltpu.VMEM((block, LANES), jnp.int32),
            pltpu.VMEM((blocks * swap_rows, LANES), jnp.int32),
            pltpu.VMEM((blocks * swap_rows, LANES), jnp.int32),
            pltpu.VMEM((half_rows, LANES), jnp.int32),
            pltpu.VMEM((half_rows, LANES), jnp.int32),
            pltpu.VMEM((2, 1, 2 * checks), jnp.int32),
            pltpu.VMEM((clients * shards, 1, 2 * checks), jnp.int32),
            pltpu.VMEM((2, 8, LANES), jnp.int32),
            dma((2, STREAMS)),
            dma((blocks,)),
            dma((blocks,)),
            dma((STREAMS, bits)),
            dma((STREAMS, bits)),
            dma((STREAMS, bits)),
            dma((STREAMS, bits)),
            dma((2,)),
            dma((2,)),
        ],
        compiler_params=pltpu.CompilerParams(collective_id=0, has_side_effects=True),
        name="aggregate_and_project",
    )(
        alive_flags,
        row_seeds,
        quantized.reshape(rows, LANES),
        pair_masks.reshape(rows, LANES),
    )


def finish_kernel(clients, packed, sums, agg_out, own_out, diff_out):
    block = agg_out.shape[0] // clients
    swap_rows = packed_rows(block)
    first = pl.program_id(0) * clients

    @pl.loop(0, clients)
    def _(n):
        def put(at, count, v):
            agg_out[pl.ds(pl.multiple_of(n * block + at, 8), count), :] = v

        unpack_block(packed, (first + n) * swap_rows, block, put)

    checks = own_out.shape[1]
    diff_out[...] = sums[:, :checks]
    own_out[...] = sums[:, checks:]


def finish(packed, sums, rows, clients):
    checks = sums.shape[1] // 2
    vmem = pl.BlockSpec(memory_space=pltpu.VMEM)
    return pl.pallas_call(
        functools.partial(finish_kernel, clients),
        grid=(STREAMS,),
        in_specs=[vmem, vmem],
        out_specs=[pl.BlockSpec((rows // STREAMS, LANES), lambda i: (i, 0)), vmem, vmem],
        out_shape=[
            jax.ShapeDtypeStruct((rows, LANES), jnp.int32),
            jax.ShapeDtypeStruct((1, checks), jnp.int32),
            jax.ShapeDtypeStruct((1, checks), jnp.int32),
        ],
        compiler_params=pltpu.CompilerParams(vmem_limit_bytes=16 * 1024 * 1024),
        name="finish",
    )(packed, sums)


def body(quantized, pair_masks, alive_flags, row_seeds):
    length = quantized.shape[1]
    clients = lax.axis_size("clients")
    shards = lax.axis_size("shard")
    packed, sums = aggregate_and_project(
        quantized, pair_masks, alive_flags, row_seeds, clients, shards
    )
    aggregate, own, diff = finish(packed, sums, length // LANES, clients)
    return (aggregate.reshape(length), own, diff.reshape(-1))


def solution(mesh):
    placed = (P("clients", "shard"), P("clients", "shard"), P("clients"), P())
    return jax.shard_map(
        body,
        mesh=mesh,
        in_specs=placed,
        out_specs=(P("shard"), P("clients", None), P()),
        check_vma=False,
    )
```

```python
import functools

import jax
import jax.numpy as jnp
from jax import lax
from jax.experimental import pallas as pl
from jax.experimental.pallas import tpu as pltpu
from jax.sharding import PartitionSpec as P

modulus = 2097143
mask21 = 2097151
LANES = 128
STREAMS = 4
AHEAD = 3
STRIDE = (LANES * 747796405 + 2147483648) % 4294967296 - 2147483648


def reduce_mod(x):
    x = (x & mask21) + (x >> 21) * 9
    return jnp.where(x >= modulus, x - modulus, x)


def wrap_once(x):
    return jnp.where(x >= modulus, x - modulus, x)


def packed_rows(count):
    tiles = count // 8
    return 8 * (2 * (tiles // 3) + tiles % 3)


def pack3(a, b, c):
    return a | (c << 21), b | ((c >> 11) << 21)


def unpack3(x, y):
    c = lax.shift_right_logical(x, 21) | ((y >> 21) << 11)
    return x & mask21, y & mask21, c


def each_step(tiles, fn):
    step = max(d for d in range(1, 9) if tiles % d == 0)

    def one(i):
        fn(i * step * 8, step * 8)

    if tiles == step:
        one(0)
    else:
        pl.loop(0, tiles // step)(one)


def pack_block(src, start, dst, at, count):
    third = 8 * (count // 24)
    rest = count - 3 * third

    def rows(x):
        return pl.multiple_of(x, 8)

    if third:

        def one(i, n):
            a = src[pl.ds(rows(start + i), n), :]
            b = src[pl.ds(rows(start + third + i), n), :]
            c = src[pl.ds(rows(start + 2 * third + i), n), :]
            x, y = pack3(a, b, c)
            dst[pl.ds(rows(at + i), n), :] = x
            dst[pl.ds(rows(at + third + i), n), :] = y

        each_step(third // 8, one)
    if rest:
        dst[pl.ds(rows(at + 2 * third), rest), :] = src[pl.ds(rows(start + 3 * third), rest), :]


def unpack_block(src, at, count, put):
    third = 8 * (count // 24)
    rest = count - 3 * third

    def rows(x):
        return pl.multiple_of(x, 8)

    if third:

        def one(i, n):
            x = src[pl.ds(rows(at + i), n), :]
            y = src[pl.ds(rows(at + third + i), n), :]
            for j, v in enumerate(unpack3(x, y)):
                put(j * third + i, n, v)

        each_step(third // 8, one)
    if rest:
        put(3 * third, rest, src[pl.ds(rows(at + 2 * third), rest), :])


def table_tile(start):
    v = start & 2147483647
    v = v ^ (v >> 15)
    v = (v * 277803737) & 2147483647
    v = v ^ (v >> 13)
    v = v * 1103515245
    v = v ^ (v >> 16)
    high = (v >> 5).astype(jnp.int8) & jnp.int8(31)
    low = v.astype(jnp.int8) & jnp.int8(31)
    return high.astype(jnp.bfloat16), low.astype(jnp.bfloat16)


def aggregate_kernel(
    clients,
    length,
    alive_ref,
    seeds_ref,
    quant_hbm,
    masks_hbm,
    gathered,
    sums_out,
    quant,
    masked,
    base,
    partner,
    swap_from,
    swap_to,
    sent,
    arrived,
    rows_out,
    rows_in,
    flags,
    load_sem,
    swap_send,
    swap_recv,
    rs_send,
    rs_recv,
    ag_send,
    ag_recv,
    flag_sem,
    sums_sem,
):
    rows = quant.shape[0]
    checks = seeds_ref.shape[0]
    devices = rows_in.shape[0]
    bits = clients.bit_length() - 1
    me = lax.axis_index("clients")
    shards = lax.axis_size("shard")
    here = lax.axis_index("shard")
    start = here * length
    alive = alive_ref[0]
    stream = rows // STREAMS
    block = stream // clients
    unit = min(128, block)
    group = min(64, unit)
    per_block = block // unit
    others = clients // 2 - 1
    blocks = STREAMS * (others + 1)
    swap_rows = packed_rows(block)
    counts = [stream >> (i + 1) for i in range(bits)]
    sizes = [packed_rows(c) for c in counts]
    offsets = [sum(sizes[:i]) for i in range(bits)]
    per_stream = sum(sizes)

    barrier = pltpu.get_barrier_semaphore()
    for b in range(bits):
        pl.semaphore_signal(barrier, inc=1, device_id={"clients": me ^ (1 << b)})
    for n in range(1, shards):
        pl.semaphore_signal(barrier, inc=1, device_id={"shard": lax.rem(here + n, shards)})
    peers = bits + shards - 1

    order = [h ^ 1 for h in range(STREAMS)]
    loads = []
    for h in range(STREAMS):
        at = pl.ds(h * stream, stream)
        loads.append(
            (
                pltpu.make_async_copy(quant_hbm.at[at], quant.at[at], load_sem.at[0, h]),
                pltpu.make_async_copy(masks_hbm.at[at], masked.at[at], load_sem.at[1, h]),
            )
        )
    for side in range(2):
        for h in order:
            loads[h][side].start()

    bit = [(me >> b) & 1 for b in range(bits)]
    share_even = sum(bit[i] << (bits - 1 - i) for i in range(bits))
    share_odd = sum(bit[(i + 1) % bits] << (bits - 1 - i) for i in range(bits))

    def share_of(h):
        return jnp.where(h % 2 == 1, share_odd, share_even)

    def partner_at(h, i):
        return me ^ jnp.where(h % 2 == 1, 1 << ((i + 1) % bits), 1 << i)

    def keep_row(h, i, flip=0):
        s = ((share_of(h) >> (bits - 1 - i)) ^ flip) << (bits - 1 - i)
        return pl.multiple_of(h * stream + s * block, 8)

    def block_row(w, flip=False):
        shared = w >= STREAMS * others
        h = w % STREAMS
        k = jnp.where(shared, 0, others - w // STREAMS)
        odd = h % 2 == 1
        k = jnp.where(odd, 2 * k, k)
        s = share_of(h) ^ k
        if flip:
            s = s ^ jnp.where(odd, 1, clients // 2)
        return pl.multiple_of(h * stream + s * block, 8)

    def swap_copy(w):
        at = pl.ds(pl.multiple_of(w * swap_rows, 8), swap_rows)
        return pltpu.make_async_remote_copy(
            src_ref=swap_from.at[at],
            dst_ref=swap_to.at[at],
            send_sem=swap_send.at[w],
            recv_sem=swap_recv.at[w],
            device_id={"clients": me ^ 1},
        )

    def rs_at(h, i):
        return pl.multiple_of(h * per_stream + offsets[i], 8)

    def rs_copy(h, i):
        at = pl.ds(rs_at(h, i), sizes[i])
        return pltpu.make_async_remote_copy(
            src_ref=sent.at[at],
            dst_ref=arrived.at[at],
            send_sem=rs_send.at[h, i],
            recv_sem=rs_recv.at[h, i],
            device_id={"clients": partner_at(h, i)},
        )

    def rs_pack(h, i):
        pack_block(masked, keep_row(h, i, 1), sent, rs_at(h, i), counts[i])

    def rs_take(h, i):
        rs_copy(h, i).wait()
        keep = keep_row(h, i)

        def put(at, n, v):
            spot = pl.ds(pl.multiple_of(keep + at, 8), n)
            masked[spot, :] = wrap_once(masked[spot, :] + v)

        unpack_block(arrived, rs_at(h, i), counts[i], put)

    def ag_slice(h, j, flip):
        s = ((share_of(h) >> j) ^ flip) << j
        at = pl.multiple_of((h * clients + s) * swap_rows, 8)
        return gathered.at[pl.ds(at, swap_rows << j)]

    def ag_copy(h, j, flip=0):
        return pltpu.make_async_remote_copy(
            src_ref=ag_slice(h, j, flip),
            dst_ref=ag_slice(h, j, flip),
            send_sem=ag_send.at[h, j],
            recv_sem=ag_recv.at[h, j],
            device_id={"clients": partner_at(h, bits - 1 - j)},
        )

    lane = lax.broadcasted_iota(jnp.int32, (8, LANES), 1)
    sub = lax.broadcasted_iota(jnp.int32, (8, LANES), 0)
    seeds = jnp.zeros((8, LANES), jnp.int32)
    for r in range(checks):
        seeds = jnp.where(lane % checks == r, seeds_ref[r], seeds)
    for g in range(LANES // 8):
        spot = start + 8 * g + sub + lane // checks * LANES
        base[pl.ds(8 * g, 8), :] = spot * 747796405 + seeds

    def swap_pack(w):
        pack_block(quant, block_row(w, True), swap_from, w * swap_rows, block)

    flags[0] = jnp.full((8, LANES), alive)
    flag_copy = pltpu.make_async_remote_copy(
        src_ref=flags.at[0],
        dst_ref=flags.at[1],
        send_sem=flag_sem.at[0],
        recv_sem=flag_sem.at[1],
        device_id={"clients": me ^ 1},
    )

    for h in order:
        loads[h][0].wait()
    pl.loop(0, AHEAD)(swap_pack)
    pl.semaphore_wait(barrier, peers)
    swap_copy(0).start()
    step = min(64, stream)
    for n, h in enumerate(order):
        loads[h][1].wait()

        @pl.loop(0, stream // step)
        def _(i, h=h):
            at = pl.ds(pl.multiple_of(h * stream + i * step, 8), step)
            s = wrap_once(wrap_once(quant[at, :] + masked[at, :]))
            masked[at, :] = s * alive

        rs_pack(h, 0)
        rs_copy(h, 0).start()
        if n == 1:
            for w in range(1, AHEAD):
                swap_copy(w).start()
    flag_copy.start()
    pl.loop(AHEAD, blocks)(swap_pack)

    empty = jnp.zeros((8, LANES), jnp.float32)
    shift = 7 * (sub & 3)
    second = sub >= 4

    def split(first_ref, a, second_ref, b):
        one = jnp.broadcast_to(first_ref[pl.ds(a, 1), :], (8, LANES))
        two = jnp.broadcast_to(second_ref[pl.ds(b, 1), :], (8, LANES))
        return ((jnp.where(second, two, one) >> shift) & 127).astype(jnp.float32)

    def work(u, total, share):
        w = u // per_block

        @pl.when(u % per_block == 0)
        def _():
            swap_copy(w).wait()

            @pl.when(w + AHEAD < blocks)
            def _():
                swap_copy(w + AHEAD).start()

            def put(at, n, v):
                partner[pl.ds(pl.multiple_of(at, 8), n), :] = v

            unpack_block(swap_to, w * swap_rows, block, put)

        inner = (u % per_block) * unit
        row = block_row(w) + inner
        for g in range(unit // group):
            tables, pieces = [], []
            for k in range(g * group, (g + 1) * group, 2):
                at = row + k
                high, low = table_tile(base[...] + at * STRIDE)
                tables.append(jnp.concatenate([high, low], 1))
                parts = [split(quant, at, partner, inner + k)]
                parts.append(split(quant, at + 1, partner, inner + k + 1))
                if share:
                    parts += [split(masked, at, masked, at + 1), empty]
                pieces.append(jnp.concatenate(parts, 0).astype(jnp.bfloat16))
            part = lax.dot_general(
                jnp.concatenate(pieces, 1),
                jnp.concatenate(tables, 0),
                (((1,), (0,)), ((), ())),
                preferred_element_type=jnp.float32,
            ).astype(jnp.int32)
            if share:
                total = reduce_mod(total + part)
            else:
                total = jnp.concatenate([reduce_mod(total[:16] + part), total[16:]], 0)
        return total

    units = blocks * per_block
    plain = STREAMS * others * per_block
    actions = bits * STREAMS
    early = units * 9 // 16
    first = min(2, early)

    def rs_stop(a):
        return first + (early - first) * a // actions

    def ag_stop(a):
        return early + (units - early) * (a + 1) // (actions - STREAMS)

    def compute(lo, hi, total, kinds):
        if "plain" in kinds:
            total = lax.fori_loop(
                lo, jnp.minimum(hi, plain), lambda u, t: work(u, t, False), total
            )
        if "share" in kinds:
            total = lax.fori_loop(
                jnp.maximum(lo, plain), hi, lambda u, t: work(u, t, True), total
            )
        return total

    total = jnp.zeros((32, 2 * LANES), jnp.int32)
    for i in range(bits):

        def turn(h, total, i=i):
            a = i * STREAMS + h
            h = h ^ 1
            lo = jnp.where(a == 0, 0, rs_stop(a - 1))
            total = compute(lo, rs_stop(a), total, ("plain",))
            rs_take(h, i)
            if i < bits - 1:
                rs_pack(h, i + 1)
                rs_copy(h, i + 1).start()
            else:
                spot = pl.multiple_of((h * clients + share_of(h)) * swap_rows, 8)
                pack_block(masked, keep_row(h, i), gathered, spot, block)
                ag_copy(h, 0).start()
            return total

        total = lax.fori_loop(0, STREAMS, turn, total)
    def gather_turn(h, j):
        ag_copy(h, j).wait_send()
        ag_copy(h, j, 1).wait_recv()
        if j < bits - 1:
            ag_copy(h, j + 1).start()

    for j in range(bits - 1):
        kinds = []
        lo_static = rs_stop(actions - 1) if j == 0 else ag_stop(j * STREAMS - 1)
        hi_static = ag_stop((j + 1) * STREAMS - 1)
        if lo_static < plain:
            kinds.append("plain")
        if hi_static > plain:
            kinds.append("share")

        def turn(h, total, j=j, kinds=tuple(kinds)):
            a = j * STREAMS + h
            h = h ^ 1
            lo = jnp.where(a == 0, rs_stop(actions - 1), ag_stop(a - 1))
            total = compute(lo, ag_stop(a), total, kinds)
            gather_turn(h, j)
            return total

        total = lax.fori_loop(0, STREAMS, turn, total)

    flag_copy.wait()
    total = reduce_mod(total[:, :LANES] * 32 + total[:, LANES:])
    moved = pltpu.roll(total, checks, 1)
    pair = total[0:8] + moved[8:16]
    whole = total[16:24] + pltpu.roll(moved[16:24], 4, 0)
    total = reduce_mod(jnp.concatenate([pair, whole], 0))

    def combine(r):
        high = reduce_mod(total[r + 2 : r + 3] * 128 + total[r + 1 : r + 2])
        return reduce_mod(high * 128 + total[r : r + 1])

    own, other = combine(0), combine(4)
    diff = combine(8) - own * alive - other * flags[1, :1]
    diff = jnp.where(diff < 0, diff + modulus, diff)
    diff = jnp.where(diff < 0, diff + modulus, diff)
    left = lax.broadcasted_iota(jnp.int32, (1, LANES), 1) < checks
    mine = jnp.where(left, diff, pltpu.roll(own, checks, 1))
    rows_out[0] = mine
    rows_out[1] = jnp.where(left, diff, pltpu.roll(other, checks, 1))
    rows_in[0] = mine

    def row_copy(n):
        return pltpu.make_async_remote_copy(
            src_ref=rows_out.at[jnp.where(n // shards == 1, 1, 0)],
            dst_ref=rows_in.at[n],
            send_sem=sums_sem.at[0],
            recv_sem=sums_sem.at[1],
            device_id={"clients": me ^ (n // shards), "shard": (here + n) % shards},
        )

    @pl.loop(1, devices)
    def _(n):
        row_copy(devices - n).start()

    @pl.loop(0, STREAMS)
    def _(h):
        gather_turn(h ^ 1, bits - 1)

    landed = rows_in.at[pl.ds(1, devices - 1)]
    pltpu.make_async_copy(landed, landed, sums_sem.at[0]).wait()
    pltpu.make_async_copy(landed, landed, sums_sem.at[1]).wait()
    near = rows_in[0]
    for n in range(1, 2 * shards):
        near = near + rows_in[n]
    every = lax.fori_loop(2 * shards, devices, lambda n, t: t + rows_in[n], near)
    sums_out[...] = reduce_mod(jnp.where(left, every, near))


def aggregate_and_project(quantized, pair_masks, alive_flags, row_seeds, clients, shards):
    length = quantized.shape[1]
    rows = length // LANES
    checks = row_seeds.shape[0]
    bits = clients.bit_length() - 1
    block = rows // STREAMS // clients
    blocks = STREAMS * clients // 2
    swap_rows = packed_rows(block)
    half_rows = STREAMS * sum(packed_rows(rows // STREAMS >> (i + 1)) for i in range(bits))
    gather_rows = STREAMS * clients * swap_rows
    vmem = pl.BlockSpec(memory_space=pltpu.VMEM)
    smem = pl.BlockSpec(memory_space=pltpu.SMEM)
    hbm = pl.BlockSpec(memory_space=pl.ANY)
    dma = pltpu.SemaphoreType.DMA
    return pl.pallas_call(
        functools.partial(aggregate_kernel, clients, length),
        in_specs=[smem, smem, hbm, hbm],
        out_specs=[vmem, vmem],
        out_shape=[
            pltpu.VMEM((gather_rows, LANES), jnp.int32),
            pltpu.VMEM((1, 2 * checks), jnp.int32),
        ],
        scratch_shapes=[
            pltpu.VMEM((rows, LANES), jnp.int32),
            pltpu.VMEM((rows, LANES), jnp.int32),
            pltpu.VMEM((LANES, LANES), jnp.int32),
            pltpu.VMEM((block, LANES), jnp.int32),
            pltpu.VMEM((blocks * swap_rows, LANES), jnp.int32),
            pltpu.VMEM((blocks * swap_rows, LANES), jnp.int32),
            pltpu.VMEM((half_rows, LANES), jnp.int32),
            pltpu.VMEM((half_rows, LANES), jnp.int32),
            pltpu.VMEM((2, 1, 2 * checks), jnp.int32),
            pltpu.VMEM((clients * shards, 1, 2 * checks), jnp.int32),
            pltpu.VMEM((2, 8, LANES), jnp.int32),
            dma((2, STREAMS)),
            dma((blocks,)),
            dma((blocks,)),
            dma((STREAMS, bits)),
            dma((STREAMS, bits)),
            dma((STREAMS, bits)),
            dma((STREAMS, bits)),
            dma((2,)),
            dma((2,)),
        ],
        compiler_params=pltpu.CompilerParams(collective_id=0, has_side_effects=True),
        name="aggregate_and_project",
    )(
        alive_flags,
        row_seeds,
        quantized.reshape(rows, LANES),
        pair_masks.reshape(rows, LANES),
    )


def finish_kernel(clients, packed, sums, agg_out, own_out, diff_out):
    block = agg_out.shape[0] // clients
    swap_rows = packed_rows(block)
    first = pl.program_id(0) * clients

    @pl.loop(0, clients)
    def _(n):
        def put(at, count, v):
            agg_out[pl.ds(pl.multiple_of(n * block + at, 8), count), :] = v

        unpack_block(packed, (first + n) * swap_rows, block, put)

    checks = own_out.shape[1]
    diff_out[...] = sums[:, :checks]
    own_out[...] = sums[:, checks:]


def finish(packed, sums, rows, clients):
    checks = sums.shape[1] // 2
    vmem = pl.BlockSpec(memory_space=pltpu.VMEM)
    return pl.pallas_call(
        functools.partial(finish_kernel, clients),
        grid=(STREAMS,),
        in_specs=[vmem, vmem],
        out_specs=[pl.BlockSpec((rows // STREAMS, LANES), lambda i: (i, 0)), vmem, vmem],
        out_shape=[
            jax.ShapeDtypeStruct((rows, LANES), jnp.int32),
            jax.ShapeDtypeStruct((1, checks), jnp.int32),
            jax.ShapeDtypeStruct((1, checks), jnp.int32),
        ],
        compiler_params=pltpu.CompilerParams(vmem_limit_bytes=16 * 1024 * 1024),
        name="finish",
    )(packed, sums)


def body(quantized, pair_masks, alive_flags, row_seeds):
    length = quantized.shape[1]
    clients = lax.axis_size("clients")
    shards = lax.axis_size("shard")
    packed, sums = aggregate_and_project(
        quantized, pair_masks, alive_flags, row_seeds, clients, shards
    )
    aggregate, own, diff = finish(packed, sums, length // LANES, clients)
    return (aggregate.reshape(length), own, diff.reshape(-1))


def solution(mesh):
    placed = (P("clients", "shard"), P("clients", "shard"), P("clients"), P())
    return jax.shard_map(
        body,
        mesh=mesh,
        in_specs=placed,
        out_specs=(P("shard"), P("clients", None), P()),
        check_vma=False,
    )
```

```python
import functools

import jax
import jax.numpy as jnp
from jax import lax
from jax.experimental import pallas as pl
from jax.experimental.pallas import tpu as pltpu
from jax.sharding import PartitionSpec as P

modulus = 2097143
mask21 = 2097151
LANES = 128
STREAMS = 4
AHEAD = 4
SPARE = 2
STRIDE = (LANES * 747796405 + 2147483648) % 4294967296 - 2147483648


def reduce_mod(x):
    x = (x & mask21) + (x >> 21) * 9
    return jnp.where(x >= modulus, x - modulus, x)


def wrap_once(x):
    return jnp.where(x >= modulus, x - modulus, x)


def packed_rows(count):
    tiles = count // 8
    return 8 * (2 * (tiles // 3) + tiles % 3)


def pack3(a, b, c):
    return a | (c << 21), b | ((c >> 11) << 21)


def unpack3(x, y):
    c = lax.shift_right_logical(x, 21) | ((y >> 21) << 11)
    return x & mask21, y & mask21, c


def each_step(tiles, fn):
    step = max(d for d in range(1, 9) if tiles % d == 0)

    def one(i):
        fn(i * step * 8, step * 8)

    if tiles == step:
        one(0)
    else:
        pl.loop(0, tiles // step)(one)


def pack_block(src, start, dst, at, count):
    third = 8 * (count // 24)
    rest = count - 3 * third

    def rows(x):
        return pl.multiple_of(x, 8)

    if third:

        def one(i, n):
            a = src[pl.ds(rows(start + i), n), :]
            b = src[pl.ds(rows(start + third + i), n), :]
            c = src[pl.ds(rows(start + 2 * third + i), n), :]
            x, y = pack3(a, b, c)
            dst[pl.ds(rows(at + i), n), :] = x
            dst[pl.ds(rows(at + third + i), n), :] = y

        each_step(third // 8, one)
    if rest:
        dst[pl.ds(rows(at + 2 * third), rest), :] = src[pl.ds(rows(start + 3 * third), rest), :]


def unpack_block(src, at, count, put):
    third = 8 * (count // 24)
    rest = count - 3 * third

    def rows(x):
        return pl.multiple_of(x, 8)

    if third:

        def one(i, n):
            x = src[pl.ds(rows(at + i), n), :]
            y = src[pl.ds(rows(at + third + i), n), :]
            for j, v in enumerate(unpack3(x, y)):
                put(j * third + i, n, v)

        each_step(third // 8, one)
    if rest:
        put(3 * third, rest, src[pl.ds(rows(at + 2 * third), rest), :])


def table_tile(start):
    v = start & 2147483647
    v = v ^ (v >> 15)
    v = (v * 277803737) & 2147483647
    v = v ^ (v >> 13)
    v = v * 1103515245
    v = v ^ (v >> 16)
    high = (v >> 5).astype(jnp.int8) & jnp.int8(31)
    low = v.astype(jnp.int8) & jnp.int8(31)
    return high.astype(jnp.bfloat16), low.astype(jnp.bfloat16)


def aggregate_kernel(
    clients,
    length,
    alive_ref,
    seeds_ref,
    quant_hbm,
    masks_hbm,
    gathered,
    sums_out,
    quant,
    masked,
    base,
    partner,
    swap_from,
    swap_to,
    sent,
    arrived,
    rows_out,
    rows_in,
    flags,
    load_sem,
    swap_send,
    swap_recv,
    rs_send,
    rs_recv,
    ag_send,
    ag_recv,
    flag_sem,
    sums_sem,
):
    rows = quant.shape[0]
    checks = seeds_ref.shape[0]
    devices = rows_in.shape[0]
    bits = clients.bit_length() - 1
    me = lax.axis_index("clients")
    shards = lax.axis_size("shard")
    here = lax.axis_index("shard")
    start = here * length
    alive = alive_ref[0]
    stream = rows // STREAMS
    block = stream // clients
    unit = min(128, block)
    group = min(64, unit)
    per_block = block // unit
    others = clients // 2 - 1
    blocks = STREAMS * (others + 1)
    swap_rows = packed_rows(block)
    counts = [stream >> (i + 1) for i in range(bits)]
    sizes = [packed_rows(c) for c in counts]
    offsets = [sum(sizes[:i]) for i in range(bits)]
    per_stream = sum(sizes)

    barrier = pltpu.get_barrier_semaphore()
    for b in range(bits):
        pl.semaphore_signal(barrier, inc=1, device_id={"clients": me ^ (1 << b)})
    for n in range(1, shards):
        pl.semaphore_signal(barrier, inc=1, device_id={"shard": lax.rem(here + n, shards)})
    peers = bits + shards - 1

    order = [h ^ 1 for h in range(STREAMS)]
    loads = []
    for h in range(STREAMS):
        at = pl.ds(h * stream, stream)
        loads.append(
            (
                pltpu.make_async_copy(quant_hbm.at[at], quant.at[at], load_sem.at[0, h]),
                pltpu.make_async_copy(masks_hbm.at[at], masked.at[at], load_sem.at[1, h]),
            )
        )
    for side in range(2):
        for h in order:
            loads[h][side].start()

    bit = [(me >> b) & 1 for b in range(bits)]
    share_even = sum(bit[i] << (bits - 1 - i) for i in range(bits))
    share_odd = sum(bit[(i + 1) % bits] << (bits - 1 - i) for i in range(bits))

    def share_of(h):
        return jnp.where(h % 2 == 1, share_odd, share_even)

    def partner_at(h, i):
        return me ^ jnp.where(h % 2 == 1, 1 << ((i + 1) % bits), 1 << i)

    def keep_row(h, i, flip=0):
        s = ((share_of(h) >> (bits - 1 - i)) ^ flip) << (bits - 1 - i)
        return pl.multiple_of(h * stream + s * block, 8)

    def block_row(w, flip=False):
        shared = w >= STREAMS * others
        h = w % STREAMS
        k = jnp.where(shared, 0, others - w // STREAMS)
        odd = h % 2 == 1
        k = jnp.where(odd, 2 * k, k)
        s = share_of(h) ^ k
        if flip:
            s = s ^ jnp.where(odd, 1, clients // 2)
        return pl.multiple_of(h * stream + s * block, 8)

    def swap_copy(w):
        at = pl.ds(pl.multiple_of(w * swap_rows, 8), swap_rows)
        return pltpu.make_async_remote_copy(
            src_ref=swap_from.at[at],
            dst_ref=swap_to.at[at],
            send_sem=swap_send.at[w],
            recv_sem=swap_recv.at[w],
            device_id={"clients": me ^ 1},
        )

    def rs_at(h, i):
        return pl.multiple_of(h * per_stream + offsets[i], 8)

    def rs_copy(h, i):
        at = pl.ds(rs_at(h, i), sizes[i])
        return pltpu.make_async_remote_copy(
            src_ref=sent.at[at],
            dst_ref=arrived.at[at],
            send_sem=rs_send.at[h, i],
            recv_sem=rs_recv.at[h, i],
            device_id={"clients": partner_at(h, i)},
        )

    def rs_pack(h, i):
        pack_block(masked, keep_row(h, i, 1), sent, rs_at(h, i), counts[i])

    def rs_take(h, i):
        rs_copy(h, i).wait()
        keep = keep_row(h, i)

        def put(at, n, v):
            spot = pl.ds(pl.multiple_of(keep + at, 8), n)
            masked[spot, :] = wrap_once(masked[spot, :] + v)

        unpack_block(arrived, rs_at(h, i), counts[i], put)

    def ag_slice(h, j, flip):
        s = ((share_of(h) >> j) ^ flip) << j
        at = pl.multiple_of((h * clients + s) * swap_rows, 8)
        return gathered.at[pl.ds(at, swap_rows << j)]

    def ag_copy(h, j, flip=0):
        return pltpu.make_async_remote_copy(
            src_ref=ag_slice(h, j, flip),
            dst_ref=ag_slice(h, j, flip),
            send_sem=ag_send.at[h, j],
            recv_sem=ag_recv.at[h, j],
            device_id={"clients": partner_at(h, bits - 1 - j)},
        )

    lane = lax.broadcasted_iota(jnp.int32, (8, LANES), 1)
    sub = lax.broadcasted_iota(jnp.int32, (8, LANES), 0)
    seeds = jnp.zeros((8, LANES), jnp.int32)
    for r in range(checks):
        seeds = jnp.where(lane % checks == r, seeds_ref[r], seeds)
    for g in range(LANES // 8):
        spot = start + 8 * g + sub + lane // checks * LANES
        base[pl.ds(8 * g, 8), :] = spot * 747796405 + seeds

    def swap_pack(w):
        pack_block(quant, block_row(w, True), swap_from, w * swap_rows, block)

    flags[0] = jnp.full((8, LANES), alive)
    flag_copy = pltpu.make_async_remote_copy(
        src_ref=flags.at[0],
        dst_ref=flags.at[1],
        send_sem=flag_sem.at[0],
        recv_sem=flag_sem.at[1],
        device_id={"clients": me ^ 1},
    )

    for h in order:
        loads[h][0].wait()
    pl.loop(0, AHEAD)(swap_pack)
    pl.semaphore_wait(barrier, peers)
    swap_copy(0).start()
    step = min(64, stream)
    for n, h in enumerate(order):
        loads[h][1].wait()

        @pl.loop(0, stream // step)
        def _(i, h=h):
            at = pl.ds(pl.multiple_of(h * stream + i * step, 8), step)
            s = wrap_once(wrap_once(quant[at, :] + masked[at, :]))
            masked[at, :] = s * alive

        rs_pack(h, 0)
        rs_copy(h, 0).start()
        if n == 1:
            for w in range(1, AHEAD):
                swap_copy(w).start()
    flag_copy.start()
    pl.loop(AHEAD, blocks)(swap_pack)

    empty = jnp.zeros((8, LANES), jnp.float32)
    shift = 7 * (sub & 3)
    second = sub >= 4

    def split(first_ref, a, second_ref, b):
        one = jnp.broadcast_to(first_ref[pl.ds(a, 1), :], (8, LANES))
        two = jnp.broadcast_to(second_ref[pl.ds(b, 1), :], (8, LANES))
        return ((jnp.where(second, two, one) >> shift) & 127).astype(jnp.float32)

    def work(u, total, share):
        w = u // per_block

        @pl.when(u % per_block == 0)
        def _():
            swap_copy(w).wait()

            @pl.when(w + AHEAD < blocks)
            def _():
                swap_copy(w + AHEAD).start()

            def put(at, n, v):
                partner[pl.ds(pl.multiple_of(at, 8), n), :] = v

            unpack_block(swap_to, w * swap_rows, block, put)

        inner = (u % per_block) * unit
        row = block_row(w) + inner
        for g in range(unit // group):
            tables, pieces = [], []
            for k in range(g * group, (g + 1) * group, 2):
                at = row + k
                high, low = table_tile(base[...] + at * STRIDE)
                tables.append(jnp.concatenate([high, low], 1))
                parts = [split(quant, at, partner, inner + k)]
                parts.append(split(quant, at + 1, partner, inner + k + 1))
                if share:
                    parts += [split(masked, at, masked, at + 1), empty]
                pieces.append(jnp.concatenate(parts, 0).astype(jnp.bfloat16))
            part = lax.dot_general(
                jnp.concatenate(pieces, 1),
                jnp.concatenate(tables, 0),
                (((1,), (0,)), ((), ())),
                preferred_element_type=jnp.float32,
            ).astype(jnp.int32)
            if share:
                total = reduce_mod(total + part)
            else:
                total = jnp.concatenate([reduce_mod(total[:16] + part), total[16:]], 0)
        return total

    units = blocks * per_block
    plain = STREAMS * others * per_block
    actions = bits * STREAMS
    early = units * 9 // 16
    first = min(2, early)

    def rs_stop(a):
        return first + (early - first) * a // actions

    def ag_stop(a):
        return early + (units - early) * (a + 1) // (actions - STREAMS + SPARE)

    def compute(lo, hi, total, kinds):
        if "plain" in kinds:
            total = lax.fori_loop(
                lo, jnp.minimum(hi, plain), lambda u, t: work(u, t, False), total
            )
        if "share" in kinds:
            total = lax.fori_loop(
                jnp.maximum(lo, plain), hi, lambda u, t: work(u, t, True), total
            )
        return total

    total = jnp.zeros((32, 2 * LANES), jnp.int32)
    for i in range(bits):

        def turn(h, total, i=i):
            a = i * STREAMS + h
            h = h ^ 1
            lo = jnp.where(a == 0, 0, rs_stop(a - 1))
            total = compute(lo, rs_stop(a), total, ("plain",))
            rs_take(h, i)
            if i < bits - 1:
                rs_pack(h, i + 1)
                rs_copy(h, i + 1).start()
            else:
                spot = pl.multiple_of((h * clients + share_of(h)) * swap_rows, 8)
                pack_block(masked, keep_row(h, i), gathered, spot, block)
                ag_copy(h, 0).start()
            return total

        total = lax.fori_loop(0, STREAMS, turn, total)
    def gather_turn(h, j):
        ag_copy(h, j).wait_send()
        ag_copy(h, j, 1).wait_recv()
        if j < bits - 1:
            ag_copy(h, j + 1).start()

    for j in range(bits - 1):
        kinds = []
        lo_static = rs_stop(actions - 1) if j == 0 else ag_stop(j * STREAMS - 1)
        hi_static = ag_stop((j + 1) * STREAMS - 1)
        if lo_static < plain:
            kinds.append("plain")
        if hi_static > plain:
            kinds.append("share")

        def turn(h, total, j=j, kinds=tuple(kinds)):
            a = j * STREAMS + h
            h = h ^ 1
            lo = jnp.where(a == 0, rs_stop(actions - 1), ag_stop(a - 1))
            total = compute(lo, ag_stop(a), total, kinds)
            gather_turn(h, j)
            return total

        total = lax.fori_loop(0, STREAMS, turn, total)

    last = ag_stop(actions - STREAMS - 1)
    kinds = ("share",) if last >= plain else ("plain", "share")
    total = compute(last, units, total, kinds)

    flag_copy.wait()
    total = reduce_mod(total[:, :LANES] * 32 + total[:, LANES:])
    moved = pltpu.roll(total, checks, 1)
    pair = total[0:8] + moved[8:16]
    whole = total[16:24] + pltpu.roll(moved[16:24], 4, 0)
    total = reduce_mod(jnp.concatenate([pair, whole], 0))

    def combine(r):
        high = reduce_mod(total[r + 2 : r + 3] * 128 + total[r + 1 : r + 2])
        return reduce_mod(high * 128 + total[r : r + 1])

    own, other = combine(0), combine(4)
    diff = combine(8) - own * alive - other * flags[1, :1]
    diff = jnp.where(diff < 0, diff + modulus, diff)
    diff = jnp.where(diff < 0, diff + modulus, diff)
    left = lax.broadcasted_iota(jnp.int32, (1, LANES), 1) < checks
    mine = jnp.where(left, diff, pltpu.roll(own, checks, 1))
    rows_out[0] = mine
    rows_out[1] = jnp.where(left, diff, pltpu.roll(other, checks, 1))
    rows_in[0] = mine

    def row_copy(n):
        return pltpu.make_async_remote_copy(
            src_ref=rows_out.at[jnp.where(n // shards == 1, 1, 0)],
            dst_ref=rows_in.at[n],
            send_sem=sums_sem.at[0],
            recv_sem=sums_sem.at[1],
            device_id={"clients": me ^ (n // shards), "shard": (here + n) % shards},
        )

    @pl.loop(1, devices)
    def _(n):
        row_copy(devices - n).start()

    @pl.loop(0, STREAMS)
    def _(h):
        gather_turn(h ^ 1, bits - 1)

    landed = rows_in.at[pl.ds(1, devices - 1)]
    pltpu.make_async_copy(landed, landed, sums_sem.at[0]).wait()
    pltpu.make_async_copy(landed, landed, sums_sem.at[1]).wait()
    near = rows_in[0]
    for n in range(1, 2 * shards):
        near = near + rows_in[n]
    every = lax.fori_loop(2 * shards, devices, lambda n, t: t + rows_in[n], near)
    sums_out[...] = reduce_mod(jnp.where(left, every, near))


def aggregate_and_project(quantized, pair_masks, alive_flags, row_seeds, clients, shards):
    length = quantized.shape[1]
    rows = length // LANES
    checks = row_seeds.shape[0]
    bits = clients.bit_length() - 1
    block = rows // STREAMS // clients
    blocks = STREAMS * clients // 2
    swap_rows = packed_rows(block)
    half_rows = STREAMS * sum(packed_rows(rows // STREAMS >> (i + 1)) for i in range(bits))
    gather_rows = STREAMS * clients * swap_rows
    vmem = pl.BlockSpec(memory_space=pltpu.VMEM)
    smem = pl.BlockSpec(memory_space=pltpu.SMEM)
    hbm = pl.BlockSpec(memory_space=pl.ANY)
    dma = pltpu.SemaphoreType.DMA
    return pl.pallas_call(
        functools.partial(aggregate_kernel, clients, length),
        in_specs=[smem, smem, hbm, hbm],
        out_specs=[vmem, vmem],
        out_shape=[
            pltpu.VMEM((gather_rows, LANES), jnp.int32),
            pltpu.VMEM((1, 2 * checks), jnp.int32),
        ],
        scratch_shapes=[
            pltpu.VMEM((rows, LANES), jnp.int32),
            pltpu.VMEM((rows, LANES), jnp.int32),
            pltpu.VMEM((LANES, LANES), jnp.int32),
            pltpu.VMEM((block, LANES), jnp.int32),
            pltpu.VMEM((blocks * swap_rows, LANES), jnp.int32),
            pltpu.VMEM((blocks * swap_rows, LANES), jnp.int32),
            pltpu.VMEM((half_rows, LANES), jnp.int32),
            pltpu.VMEM((half_rows, LANES), jnp.int32),
            pltpu.VMEM((2, 1, 2 * checks), jnp.int32),
            pltpu.VMEM((clients * shards, 1, 2 * checks), jnp.int32),
            pltpu.VMEM((2, 8, LANES), jnp.int32),
            dma((2, STREAMS)),
            dma((blocks,)),
            dma((blocks,)),
            dma((STREAMS, bits)),
            dma((STREAMS, bits)),
            dma((STREAMS, bits)),
            dma((STREAMS, bits)),
            dma((2,)),
            dma((2,)),
        ],
        compiler_params=pltpu.CompilerParams(collective_id=0, has_side_effects=True),
        name="aggregate_and_project",
    )(
        alive_flags,
        row_seeds,
        quantized.reshape(rows, LANES),
        pair_masks.reshape(rows, LANES),
    )


def finish_kernel(clients, packed, sums, agg_out, own_out, diff_out):
    block = agg_out.shape[0] // clients
    swap_rows = packed_rows(block)
    first = pl.program_id(0) * clients

    @pl.loop(0, clients)
    def _(n):
        def put(at, count, v):
            agg_out[pl.ds(pl.multiple_of(n * block + at, 8), count), :] = v

        unpack_block(packed, (first + n) * swap_rows, block, put)

    checks = own_out.shape[1]
    diff_out[...] = sums[:, :checks]
    own_out[...] = sums[:, checks:]


def finish(packed, sums, rows, clients):
    checks = sums.shape[1] // 2
    vmem = pl.BlockSpec(memory_space=pltpu.VMEM)
    return pl.pallas_call(
        functools.partial(finish_kernel, clients),
        grid=(STREAMS,),
        in_specs=[vmem, vmem],
        out_specs=[pl.BlockSpec((rows // STREAMS, LANES), lambda i: (i, 0)), vmem, vmem],
        out_shape=[
            jax.ShapeDtypeStruct((rows, LANES), jnp.int32),
            jax.ShapeDtypeStruct((1, checks), jnp.int32),
            jax.ShapeDtypeStruct((1, checks), jnp.int32),
        ],
        compiler_params=pltpu.CompilerParams(vmem_limit_bytes=16 * 1024 * 1024),
        name="finish",
    )(packed, sums)


def body(quantized, pair_masks, alive_flags, row_seeds):
    length = quantized.shape[1]
    clients = lax.axis_size("clients")
    shards = lax.axis_size("shard")
    packed, sums = aggregate_and_project(
        quantized, pair_masks, alive_flags, row_seeds, clients, shards
    )
    aggregate, own, diff = finish(packed, sums, length // LANES, clients)
    return (aggregate.reshape(length), own, diff.reshape(-1))


def solution(mesh):
    placed = (P("clients", "shard"), P("clients", "shard"), P("clients"), P())
    return jax.shard_map(
        body,
        mesh=mesh,
        in_specs=placed,
        out_specs=(P("shard"), P("clients", None), P()),
        check_vma=False,
    )
```

```python
import functools

import jax
import jax.numpy as jnp
from jax import lax
from jax.experimental import pallas as pl
from jax.experimental.pallas import tpu as pltpu
from jax.sharding import PartitionSpec as P

modulus = 2097143
mask21 = 2097151
LANES = 128
STREAMS = 4
AHEAD = 3
STRIDE = (LANES * 747796405 + 2147483648) % 4294967296 - 2147483648


def reduce_mod(x):
    x = (x & mask21) + (x >> 21) * 9
    return jnp.where(x >= modulus, x - modulus, x)


def wrap_once(x):
    return jnp.where(x >= modulus, x - modulus, x)


def packed_rows(count):
    tiles = count // 8
    return 8 * (2 * (tiles // 3) + tiles % 3)


def pack3(a, b, c):
    return a | (c << 21), b | ((c >> 11) << 21)


def unpack3(x, y):
    c = lax.shift_right_logical(x, 21) | ((y >> 21) << 11)
    return x & mask21, y & mask21, c


def each_step(tiles, fn):
    step = max(d for d in range(1, 9) if tiles % d == 0)

    def one(i):
        fn(i * step * 8, step * 8)

    if tiles == step:
        one(0)
    else:
        pl.loop(0, tiles // step)(one)


def pack_block(src, start, dst, at, count):
    third = 8 * (count // 24)
    rest = count - 3 * third

    def rows(x):
        return pl.multiple_of(x, 8)

    if third:

        def one(i, n):
            a = src[pl.ds(rows(start + i), n), :]
            b = src[pl.ds(rows(start + third + i), n), :]
            c = src[pl.ds(rows(start + 2 * third + i), n), :]
            x, y = pack3(a, b, c)
            dst[pl.ds(rows(at + i), n), :] = x
            dst[pl.ds(rows(at + third + i), n), :] = y

        each_step(third // 8, one)
    if rest:
        dst[pl.ds(rows(at + 2 * third), rest), :] = src[pl.ds(rows(start + 3 * third), rest), :]


def unpack_block(src, at, count, put):
    third = 8 * (count // 24)
    rest = count - 3 * third

    def rows(x):
        return pl.multiple_of(x, 8)

    if third:

        def one(i, n):
            x = src[pl.ds(rows(at + i), n), :]
            y = src[pl.ds(rows(at + third + i), n), :]
            for j, v in enumerate(unpack3(x, y)):
                put(j * third + i, n, v)

        each_step(third // 8, one)
    if rest:
        put(3 * third, rest, src[pl.ds(rows(at + 2 * third), rest), :])


def table_tile(start):
    v = start & 2147483647
    v = v ^ (v >> 15)
    v = (v * 277803737) & 2147483647
    v = v ^ (v >> 13)
    v = v * 1103515245
    v = v ^ (v >> 16)
    high = (v >> 5).astype(jnp.int8) & jnp.int8(31)
    low = v.astype(jnp.int8) & jnp.int8(31)
    return high.astype(jnp.bfloat16), low.astype(jnp.bfloat16)


def aggregate_kernel(
    clients,
    length,
    alive_ref,
    seeds_ref,
    quant_hbm,
    masks_hbm,
    gathered,
    sums_out,
    quant,
    masked,
    base,
    partner,
    swap_from,
    swap_to,
    sent,
    arrived,
    rows_out,
    rows_in,
    flags,
    load_sem,
    swap_send,
    swap_recv,
    rs_send,
    rs_recv,
    ag_send,
    ag_recv,
    flag_sem,
    sums_sem,
):
    rows = quant.shape[0]
    checks = seeds_ref.shape[0]
    devices = rows_in.shape[0]
    bits = clients.bit_length() - 1
    me = lax.axis_index("clients")
    shards = lax.axis_size("shard")
    here = lax.axis_index("shard")
    start = here * length
    alive = alive_ref[0]
    stream = rows // STREAMS
    block = stream // clients
    unit = min(128, block)
    group = min(64, unit)
    per_block = block // unit
    others = clients // 2 - 1
    blocks = STREAMS * (others + 1)
    swap_rows = packed_rows(block)
    counts = [stream >> (i + 1) for i in range(bits)]
    sizes = [packed_rows(c) for c in counts]
    offsets = [sum(sizes[:i]) for i in range(bits)]
    per_stream = sum(sizes)

    barrier = pltpu.get_barrier_semaphore()
    for b in range(bits):
        pl.semaphore_signal(barrier, inc=1, device_id={"clients": me ^ (1 << b)})
    for n in range(1, shards):
        pl.semaphore_signal(barrier, inc=1, device_id={"shard": lax.rem(here + n, shards)})
    peers = bits + shards - 1

    order = [h ^ 1 for h in range(STREAMS)]
    loads = []
    for h in range(STREAMS):
        at = pl.ds(h * stream, stream)
        loads.append(
            (
                pltpu.make_async_copy(quant_hbm.at[at], quant.at[at], load_sem.at[0, h]),
                pltpu.make_async_copy(masks_hbm.at[at], masked.at[at], load_sem.at[1, h]),
            )
        )
    for side in range(2):
        for h in order:
            loads[h][side].start()

    bit = [(me >> b) & 1 for b in range(bits)]
    share_even = sum(bit[i] << (bits - 1 - i) for i in range(bits))
    share_odd = sum(bit[(i + 1) % bits] << (bits - 1 - i) for i in range(bits))

    def share_of(h):
        return jnp.where(h % 2 == 1, share_odd, share_even)

    def partner_at(h, i):
        return me ^ jnp.where(h % 2 == 1, 1 << ((i + 1) % bits), 1 << i)

    def keep_row(h, i, flip=0):
        s = ((share_of(h) >> (bits - 1 - i)) ^ flip) << (bits - 1 - i)
        return pl.multiple_of(h * stream + s * block, 8)

    def block_row(w, flip=False):
        shared = w >= STREAMS * others
        h = w % STREAMS
        k = jnp.where(shared, 0, others - w // STREAMS)
        odd = h % 2 == 1
        k = jnp.where(odd, 2 * k, k)
        s = share_of(h) ^ k
        if flip:
            s = s ^ jnp.where(odd, 1, clients // 2)
        return pl.multiple_of(h * stream + s * block, 8)

    def swap_copy(w):
        at = pl.ds(pl.multiple_of(w * swap_rows, 8), swap_rows)
        return pltpu.make_async_remote_copy(
            src_ref=swap_from.at[at],
            dst_ref=swap_to.at[at],
            send_sem=swap_send.at[w],
            recv_sem=swap_recv.at[w],
            device_id={"clients": me ^ 1},
        )

    def rs_at(h, i):
        return pl.multiple_of(h * per_stream + offsets[i], 8)

    def rs_copy(h, i):
        at = pl.ds(rs_at(h, i), sizes[i])
        return pltpu.make_async_remote_copy(
            src_ref=sent.at[at],
            dst_ref=arrived.at[at],
            send_sem=rs_send.at[h, i],
            recv_sem=rs_recv.at[h, i],
            device_id={"clients": partner_at(h, i)},
        )

    def rs_pack(h, i):
        pack_block(masked, keep_row(h, i, 1), sent, rs_at(h, i), counts[i])

    def rs_take(h, i):
        rs_copy(h, i).wait()
        keep = keep_row(h, i)

        def put(at, n, v):
            spot = pl.ds(pl.multiple_of(keep + at, 8), n)
            masked[spot, :] = wrap_once(masked[spot, :] + v)

        unpack_block(arrived, rs_at(h, i), counts[i], put)

    def ag_slice(h, j, flip):
        s = ((share_of(h) >> j) ^ flip) << j
        at = pl.multiple_of((h * clients + s) * swap_rows, 8)
        return gathered.at[pl.ds(at, swap_rows << j)]

    def ag_copy(h, j, flip=0):
        return pltpu.make_async_remote_copy(
            src_ref=ag_slice(h, j, flip),
            dst_ref=ag_slice(h, j, flip),
            send_sem=ag_send.at[h, j],
            recv_sem=ag_recv.at[h, j],
            device_id={"clients": partner_at(h, bits - 1 - j)},
        )

    lane = lax.broadcasted_iota(jnp.int32, (8, LANES), 1)
    sub = lax.broadcasted_iota(jnp.int32, (8, LANES), 0)
    seeds = jnp.zeros((8, LANES), jnp.int32)
    for r in range(checks):
        seeds = jnp.where(lane % checks == r, seeds_ref[r], seeds)
    for g in range(LANES // 8):
        spot = start + 8 * g + sub + lane // checks * LANES
        base[pl.ds(8 * g, 8), :] = spot * 747796405 + seeds

    def swap_pack(w):
        pack_block(quant, block_row(w, True), swap_from, w * swap_rows, block)

    flags[0] = jnp.full((8, LANES), alive)
    flag_copy = pltpu.make_async_remote_copy(
        src_ref=flags.at[0],
        dst_ref=flags.at[1],
        send_sem=flag_sem.at[0],
        recv_sem=flag_sem.at[1],
        device_id={"clients": me ^ 1},
    )

    for h in order:
        loads[h][0].wait()
    pl.loop(0, AHEAD)(swap_pack)
    pl.semaphore_wait(barrier, peers)
    swap_copy(0).start()
    step = min(64, stream)
    for n, h in enumerate(order):
        loads[h][1].wait()

        @pl.loop(0, stream // step)
        def _(i, h=h):
            at = pl.ds(pl.multiple_of(h * stream + i * step, 8), step)
            s = wrap_once(wrap_once(quant[at, :] + masked[at, :]))
            masked[at, :] = s * alive

        rs_pack(h, 0)
        rs_copy(h, 0).start()
        if n == 1:
            for w in range(1, AHEAD):
                swap_copy(w).start()
    flag_copy.start()
    pl.loop(AHEAD, blocks)(swap_pack)

    empty = jnp.zeros((8, LANES), jnp.float32)
    shift = 7 * (sub & 3)
    second = sub >= 4

    def split(first_ref, a, second_ref, b):
        one = jnp.broadcast_to(first_ref[pl.ds(a, 1), :], (8, LANES))
        two = jnp.broadcast_to(second_ref[pl.ds(b, 1), :], (8, LANES))
        return ((jnp.where(second, two, one) >> shift) & 127).astype(jnp.float32)

    def work(u, total, share):
        w = u // per_block

        @pl.when(u % per_block == 0)
        def _():
            swap_copy(w).wait()

            @pl.when(w + AHEAD < blocks)
            def _():
                swap_copy(w + AHEAD).start()

            def put(at, n, v):
                partner[pl.ds(pl.multiple_of(at, 8), n), :] = v

            unpack_block(swap_to, w * swap_rows, block, put)

        inner = (u % per_block) * unit
        row = block_row(w) + inner
        for g in range(unit // group):
            tables, pieces = [], []
            for k in range(g * group, (g + 1) * group, 2):
                at = row + k
                high, low = table_tile(base[...] + at * STRIDE)
                tables.append(jnp.concatenate([high, low], 1))
                parts = [split(quant, at, partner, inner + k)]
                parts.append(split(quant, at + 1, partner, inner + k + 1))
                if share:
                    parts += [split(masked, at, masked, at + 1), empty]
                pieces.append(jnp.concatenate(parts, 0).astype(jnp.bfloat16))
            part = lax.dot_general(
                jnp.concatenate(pieces, 1),
                jnp.concatenate(tables, 0),
                (((1,), (0,)), ((), ())),
                preferred_element_type=jnp.float32,
            ).astype(jnp.int32)
            if share:
                total = reduce_mod(total + part)
            else:
                total = jnp.concatenate([reduce_mod(total[:16] + part), total[16:]], 0)
        return total

    units = blocks * per_block
    plain = STREAMS * others * per_block
    actions = bits * STREAMS
    early = units * 9 // 16
    first = min(2, early)

    def rs_stop(a):
        return first + (early - first) * a // actions

    def ag_stop(a):
        return early + (units - early) * (a + 1) // (actions - STREAMS)

    def compute(lo, hi, total, kinds):
        if "plain" in kinds:
            total = lax.fori_loop(
                lo, jnp.minimum(hi, plain), lambda u, t: work(u, t, False), total
            )
        if "share" in kinds:
            total = lax.fori_loop(
                jnp.maximum(lo, plain), hi, lambda u, t: work(u, t, True), total
            )
        return total

    total = jnp.zeros((32, 2 * LANES), jnp.int32)
    for i in range(bits):

        def turn(h, total, i=i):
            a = i * STREAMS + h
            h = h ^ 1
            lo = jnp.where(a == 0, 0, rs_stop(a - 1))
            total = compute(lo, rs_stop(a), total, ("plain",))
            rs_take(h, i)
            if i < bits - 1:
                rs_pack(h, i + 1)
                rs_copy(h, i + 1).start()
            else:
                spot = pl.multiple_of((h * clients + share_of(h)) * swap_rows, 8)
                pack_block(masked, keep_row(h, i), gathered, spot, block)
                ag_copy(h, 0).start()
            return total

        total = lax.fori_loop(0, STREAMS, turn, total)
    def gather_turn(h, j):
        ag_copy(h, j).wait_send()
        ag_copy(h, j, 1).wait_recv()
        if j < bits - 1:
            ag_copy(h, j + 1).start()

    for j in range(bits - 1):
        kinds = []
        lo_static = rs_stop(actions - 1) if j == 0 else ag_stop(j * STREAMS - 1)
        hi_static = ag_stop((j + 1) * STREAMS - 1)
        if lo_static < plain:
            kinds.append("plain")
        if hi_static > plain:
            kinds.append("share")

        def turn(h, total, j=j, kinds=tuple(kinds)):
            a = j * STREAMS + h
            h = h ^ 1
            lo = jnp.where(a == 0, rs_stop(actions - 1), ag_stop(a - 1))
            total = compute(lo, ag_stop(a), total, kinds)
            gather_turn(h, j)
            return total

        total = lax.fori_loop(0, STREAMS, turn, total)

    flag_copy.wait()
    total = reduce_mod(total[:, :LANES] * 32 + total[:, LANES:])
    moved = pltpu.roll(total, checks, 1)
    pair = total[0:8] + moved[8:16]
    whole = total[16:24] + pltpu.roll(moved[16:24], 4, 0)
    total = reduce_mod(jnp.concatenate([pair, whole], 0))

    def combine(r):
        high = reduce_mod(total[r + 2 : r + 3] * 128 + total[r + 1 : r + 2])
        return reduce_mod(high * 128 + total[r : r + 1])

    own, other = combine(0), combine(4)
    diff = combine(8) - own * alive - other * flags[1, :1]
    diff = jnp.where(diff < 0, diff + modulus, diff)
    diff = jnp.where(diff < 0, diff + modulus, diff)
    left = lax.broadcasted_iota(jnp.int32, (1, LANES), 1) < checks
    mine = jnp.where(left, diff, pltpu.roll(own, checks, 1))
    rows_out[0] = mine
    rows_out[1] = jnp.where(left, diff, pltpu.roll(other, checks, 1))
    rows_in[0] = mine

    def row_copy(n):
        return pltpu.make_async_remote_copy(
            src_ref=rows_out.at[jnp.where(n // shards == 1, 1, 0)],
            dst_ref=rows_in.at[n],
            send_sem=sums_sem.at[0],
            recv_sem=sums_sem.at[1],
            device_id={"clients": me ^ (n // shards), "shard": (here + n) % shards},
        )

    @pl.loop(1, devices)
    def _(n):
        row_copy(devices - n).start()

    @pl.loop(0, STREAMS)
    def _(h):
        gather_turn(h ^ 1, bits - 1)

    landed = rows_in.at[pl.ds(1, devices - 1)]
    pltpu.make_async_copy(landed, landed, sums_sem.at[0]).wait()
    pltpu.make_async_copy(landed, landed, sums_sem.at[1]).wait()
    near = rows_in[0]
    for n in range(1, 2 * shards):
        near = near + rows_in[n]
    every = jnp.sum(rows_in[...], axis=0)
    sums_out[...] = reduce_mod(jnp.where(left, every, near))


def aggregate_and_project(quantized, pair_masks, alive_flags, row_seeds, clients, shards):
    length = quantized.shape[1]
    rows = length // LANES
    checks = row_seeds.shape[0]
    bits = clients.bit_length() - 1
    block = rows // STREAMS // clients
    blocks = STREAMS * clients // 2
    swap_rows = packed_rows(block)
    half_rows = STREAMS * sum(packed_rows(rows // STREAMS >> (i + 1)) for i in range(bits))
    gather_rows = STREAMS * clients * swap_rows
    vmem = pl.BlockSpec(memory_space=pltpu.VMEM)
    smem = pl.BlockSpec(memory_space=pltpu.SMEM)
    hbm = pl.BlockSpec(memory_space=pl.ANY)
    dma = pltpu.SemaphoreType.DMA
    return pl.pallas_call(
        functools.partial(aggregate_kernel, clients, length),
        in_specs=[smem, smem, hbm, hbm],
        out_specs=[vmem, vmem],
        out_shape=[
            pltpu.VMEM((gather_rows, LANES), jnp.int32),
            pltpu.VMEM((1, 2 * checks), jnp.int32),
        ],
        scratch_shapes=[
            pltpu.VMEM((rows, LANES), jnp.int32),
            pltpu.VMEM((rows, LANES), jnp.int32),
            pltpu.VMEM((LANES, LANES), jnp.int32),
            pltpu.VMEM((block, LANES), jnp.int32),
            pltpu.VMEM((blocks * swap_rows, LANES), jnp.int32),
            pltpu.VMEM((blocks * swap_rows, LANES), jnp.int32),
            pltpu.VMEM((half_rows, LANES), jnp.int32),
            pltpu.VMEM((half_rows, LANES), jnp.int32),
            pltpu.VMEM((2, 1, 2 * checks), jnp.int32),
            pltpu.VMEM((clients * shards, 1, 2 * checks), jnp.int32),
            pltpu.VMEM((2, 8, LANES), jnp.int32),
            dma((2, STREAMS)),
            dma((blocks,)),
            dma((blocks,)),
            dma((STREAMS, bits)),
            dma((STREAMS, bits)),
            dma((STREAMS, bits)),
            dma((STREAMS, bits)),
            dma((2,)),
            dma((2,)),
        ],
        compiler_params=pltpu.CompilerParams(collective_id=0, has_side_effects=True),
        name="aggregate_and_project",
    )(
        alive_flags,
        row_seeds,
        quantized.reshape(rows, LANES),
        pair_masks.reshape(rows, LANES),
    )


def finish_kernel(clients, packed, sums, agg_out, own_out, diff_out):
    block = agg_out.shape[0] // clients
    swap_rows = packed_rows(block)
    first = pl.program_id(0) * clients

    @pl.loop(0, clients)
    def _(n):
        def put(at, count, v):
            agg_out[pl.ds(pl.multiple_of(n * block + at, 8), count), :] = v

        unpack_block(packed, (first + n) * swap_rows, block, put)

    checks = own_out.shape[1]
    diff_out[...] = sums[:, :checks]
    own_out[...] = sums[:, checks:]


def finish(packed, sums, rows, clients):
    checks = sums.shape[1] // 2
    vmem = pl.BlockSpec(memory_space=pltpu.VMEM)
    return pl.pallas_call(
        functools.partial(finish_kernel, clients),
        grid=(STREAMS,),
        in_specs=[vmem, vmem],
        out_specs=[pl.BlockSpec((rows // STREAMS, LANES), lambda i: (i, 0)), vmem, vmem],
        out_shape=[
            jax.ShapeDtypeStruct((rows, LANES), jnp.int32),
            jax.ShapeDtypeStruct((1, checks), jnp.int32),
            jax.ShapeDtypeStruct((1, checks), jnp.int32),
        ],
        compiler_params=pltpu.CompilerParams(vmem_limit_bytes=16 * 1024 * 1024),
        name="finish",
    )(packed, sums)


def body(quantized, pair_masks, alive_flags, row_seeds):
    length = quantized.shape[1]
    clients = lax.axis_size("clients")
    shards = lax.axis_size("shard")
    packed, sums = aggregate_and_project(
        quantized, pair_masks, alive_flags, row_seeds, clients, shards
    )
    aggregate, own, diff = finish(packed, sums, length // LANES, clients)
    return (aggregate.reshape(length), own, diff.reshape(-1))


def solution(mesh):
    placed = (P("clients", "shard"), P("clients", "shard"), P("clients"), P())
    return jax.shard_map(
        body,
        mesh=mesh,
        in_specs=placed,
        out_specs=(P("shard"), P("clients", None), P()),
        check_vma=False,
    )
```
